32 devices in a mesh: grp: 2 (over x), rep: 4 (over z), tp: 4 (over y, core).
Axes of the slice: x: 2, y: 2, z: 4, core: 2. Of those that a mesh axis runs over, the one named last changes fastest.
Arguments:
- grad_parts: float32 [4, 5120, 2048], P('tp', ('grp', 'rep')), may hold values from -124 to 124
- master: float32 [5120, 2048], P(('grp', 'rep'), 'tp'), may hold values from -0.078125 to 0.078125
- moment_one: float32 [5120, 2048], P(('grp', 'rep'), 'tp'), may hold values from -1.5 to 1.5
- moment_two: float32 [5120, 2048], P(('grp', 'rep'), 'tp'), may hold values from 0.003 to 0.03
- hidden_in: bfloat16 [32, 4, 5120], P(('grp', 'rep')), may hold values from -6 to 6
- queries: bfloat16 [32, 4, 5120], P(('grp', 'rep'), None, 'tp'), may hold values from -8 to 8
- cache_keys: bfloat16 [32, 1024, 1024], P(('grp', 'rep'), None, 'tp'), may hold values from -8 to 8
- cache_values: bfloat16 [32, 1024, 1024], P(('grp', 'rep'), None, 'tp'), may hold values from -6 to 6
- cache_lengths: int32 [32], P(('grp', 'rep')), may hold values from 16 to 1024
Outputs:
- new_moment_one: float32 [5120, 2048], P(('grp', 'rep'), 'tp')
- new_moment_two: float32 [5120, 2048], P(('grp', 'rep'), 'tp')
- new_entries: bfloat16 [32, 4, 2048], P(('grp', 'rep'), None, 'tp')
- attended: bfloat16 [32, 4, 5120], P(('grp', 'rep'), None, 'tp')
The draws below stay inside these ranges and needn't reach their ends.
Inputs may be any that keep to these rules, and one draw needn't show every extreme that they name: `cache_lengths`: cache slots at or after a row's length hold no part of its cache.
All inputs are finite; a program needn't handle non-finite values.
Results may differ from the reference program's by a relative error of at most 0.0051.
Values may be sent and summed in bfloat16 or wider, within the bound.
A program may use at most 64 MiB of HBM per device.

```python
import math
import jax
import jax.numpy as jnp
from jax import lax

D = 5120
QH = 40
KVH = 8
HD = 128
CACHE = 1024
STEPS = 4
ROWS = 32
N_GRP = 2
N_REP = 4
N_TP = 4


def grad_levels(key):
    block_rows = D // (N_GRP * N_REP)
    row_power = jax.random.uniform(jax.random.fold_in(key, 34), (N_GRP * N_REP,), jnp.float32, -0.5, 0.0)
    row_level = jnp.repeat(jnp.exp(math.log(10.0) * row_power), block_rows)
    col_power = jax.random.uniform(jax.random.fold_in(key, 35), (2 * KVH,), jnp.float32, -1.0, 0.0)
    col_level = jnp.repeat(jnp.exp(math.log(10.0) * col_power), HD)
    return row_level[None, :, None] * col_level[None, None, :]


def draw_grad_parts(key, part):
    data_index = jnp.arange(N_TP, dtype=jnp.float32)
    row_index = jnp.arange(D, dtype=jnp.float32)
    growth = (1.0 + 2.0 * data_index / (N_TP - 1))[:, None, None] * (1.0 + 2.0 * row_index / (D - 1))[None, :, None]
    growth = growth * grad_levels(key)
    shape = (N_TP, D, 2 * KVH * HD)
    noise = jax.random.truncated_normal(jax.random.fold_in(key, 33), -6.0, 6.0, shape, jnp.float32)
    return noise * growth


def draw_queries(key, part):
    shape = (ROWS, STEPS, QH * HD)
    return jax.random.truncated_normal(jax.random.fold_in(key, 42), -6.0, 6.0, shape, jnp.float32).astype(jnp.bfloat16)


def draw_cache_keys(key, part):
    shape = (ROWS, CACHE, KVH * HD)
    return jax.random.truncated_normal(jax.random.fold_in(key, 52), -6.0, 6.0, shape, jnp.float32).astype(jnp.bfloat16)


def plant(values, key, smallest, top_value):
    longest = values.shape.index(max(values.shape))
    spots = []
    for shift in (0, 1):
        where = [jax.random.randint(jax.random.fold_in(key, axis), (), 0, length) for axis, length in enumerate(values.shape)]
        where[longest] = (where[longest] + shift) % values.shape[longest]
        spots.append(tuple(where))
    return values.at[spots[0]].set(smallest).at[spots[1]].set(top_value)


def block_scale(stream_key, shape, cuts, least, largest):
    gain, own = 1.0, jax.random.fold_in(stream_key, 6)
    for position, parts in cuts:
        draws = jnp.exp(jax.random.uniform(jax.random.fold_in(own, position), (parts,), jnp.float32, least / len(cuts), largest / len(cuts)))
        gain = gain * jnp.repeat(draws, shape[position] // parts).reshape([-1 if axis == position else 1 for axis in range(len(shape))])
    return gain


def scatter_about(own_key, dims, scale, reach, pieces=(), held_as=jnp.bfloat16):
    entries = scale * jax.random.normal(own_key, dims, jnp.float32)
    if pieces:
        entries = entries * block_scale(own_key, dims, pieces, -0.22, 0.18)
    return jnp.clip(entries, -reach, reach).astype(held_as)


def setup_inputs(seed: int = 0) -> dict:
    splits = jax.random.split(jax.random.key(seed), 10)
    return {
        "grad_parts": draw_grad_parts(jax.random.fold_in(splits[9], 71), 0),
        "master": scatter_about(splits[1], (D, 2 * KVH * HD), D ** -0.5, 0.078125, ((0, 8), (1, 4)), jnp.float32),
        "moment_one": scatter_about(splits[2], (D, 2 * KVH * HD), 0.1, 1.5, ((0, 8), (1, 4)), jnp.float32),
        "moment_two": jnp.clip(jnp.exp(math.log(0.03) - 2.3025851 * jax.random.uniform(splits[3], (D, 2 * KVH * HD), jnp.float32) ** block_scale(splits[3], (D, 2 * KVH * HD), ((0, 8), (1, 4)), -0.2, 0.2)), 0.003, 0.03),
        "hidden_in": scatter_about(splits[4], (ROWS, STEPS, D), 1.0, 6.0, ((0, 8),)),
        "queries": draw_queries(jax.random.fold_in(splits[9], 71), 0),
        "cache_keys": draw_cache_keys(jax.random.fold_in(splits[9], 71), 0),
        "cache_values": scatter_about(splits[7], (ROWS, CACHE, KVH * HD), 1.0, 6.0, ((0, 8), (2, 4))),
        "cache_lengths": plant(jax.random.randint(splits[8], (ROWS,), 16, CACHE + 1), jax.random.fold_in(splits[8], 1), 16, CACHE).astype(jnp.int32),
    }


BETA_ONE = 0.9
BETA_TWO = 0.999
FIRST_CORR = 0.9999734386011124
SECOND_CORR = 0.09520785288629041
LEARN_RATE = 0.003
EPSILON = 1e-08
ROPE_BASE = 1000000.0
NEG_FILL = -1e+30

def rotate(new_keys, lengths):
    positions = (lengths[:, None] + jnp.arange(new_keys.shape[1], dtype=jnp.int32)[None, :]).astype(jnp.float32)
    half_dim = new_keys.shape[-1] // 2
    inverse = jnp.exp(-math.log(ROPE_BASE) * 2.0 * jnp.arange(half_dim, dtype=jnp.float32) / new_keys.shape[-1])
    angles = positions[:, :, None] * inverse[None, None, :]
    cosine_part = jnp.concatenate([jnp.cos(angles), jnp.cos(angles)], -1)[:, :, None, :]
    sine_part = jnp.concatenate([jnp.sin(angles), jnp.sin(angles)], -1)[:, :, None, :]
    rotated = jnp.concatenate([-new_keys[..., half_dim:], new_keys[..., :half_dim]], -1)
    return new_keys * cosine_part + rotated * sine_part

def attend_row(items):
    query_row, old_keys, old_values, length, new_keys, new_values = items
    groups = QH // KVH
    query_heads = query_row.reshape(STEPS, KVH, groups, HD).astype(jnp.float32)
    old_k = old_keys.reshape(CACHE, KVH, HD).astype(jnp.float32)
    old_v = old_values.reshape(CACHE, KVH, HD).astype(jnp.float32)
    scaling = 1.0 / math.sqrt(HD)
    old_scores = jnp.einsum('sagd,jad->sagj', query_heads, old_k) * scaling
    valid_slots = jnp.arange(CACHE, dtype=jnp.int32) < length
    old_scores = jnp.where(valid_slots[None, None, None, :], old_scores, NEG_FILL)
    new_scores = jnp.einsum('sagd,tad->sagt', query_heads, new_keys.astype(jnp.float32)) * scaling
    causal = jnp.arange(STEPS)[:, None] >= jnp.arange(STEPS)[None, :]
    new_scores = jnp.where(causal[:, None, None, :], new_scores, NEG_FILL)
    scores = jnp.concatenate([old_scores, new_scores], -1)
    row_max = lax.optimization_barrier(jnp.max(scores, -1, keepdims=True))
    exp_scores = jnp.exp(scores - row_max)
    probs = (exp_scores / lax.optimization_barrier(jnp.sum(exp_scores, -1, keepdims=True))).astype(jnp.bfloat16)
    output = jnp.einsum('sagj,jad->sagd', probs[..., :CACHE].astype(jnp.float32), old_v)
    output = output + jnp.einsum('sagt,tad->sagd', probs[..., CACHE:].astype(jnp.float32), new_values.astype(jnp.float32))
    return output.reshape(STEPS, QH * HD).astype(jnp.bfloat16)

def reference(grad_parts, master, moment_one, moment_two, hidden_in, queries, cache_keys, cache_values, cache_lengths):
    grad_sum = lax.optimization_barrier(jnp.sum(grad_parts, axis=0))
    squares = jnp.sum(grad_sum * grad_sum)
    norm_limit = math.sqrt(D * 2 * KVH * HD)
    clipped = grad_sum * jnp.minimum(1.0, norm_limit / jnp.sqrt(squares))
    new_moment_one = BETA_ONE * moment_one + (1.0 - BETA_ONE) * clipped
    new_moment_two = BETA_TWO * moment_two + (1.0 - BETA_TWO) * clipped * clipped
    update = new_moment_one / FIRST_CORR / (jnp.sqrt(new_moment_two / SECOND_CORR) + EPSILON)
    weights = (master - LEARN_RATE * update).astype(jnp.bfloat16)
    projected = jnp.dot(hidden_in.reshape(ROWS * STEPS, D), weights, preferred_element_type=jnp.float32)
    projected = projected.reshape(ROWS, STEPS, KVH, 2, HD)
    new_keys = rotate(projected[:, :, :, 0, :], cache_lengths).astype(jnp.bfloat16)
    new_values = projected[:, :, :, 1, :].astype(jnp.bfloat16)
    new_entries = jnp.stack([new_keys, new_values], 3).reshape(ROWS, STEPS, 2 * KVH * HD)
    attended = lax.map(attend_row, (queries, cache_keys, cache_values, cache_lengths, new_keys, new_values))
    return (new_moment_one, new_moment_two, new_entries, attended)
```

```python
import functools
import math

import jax
import jax.numpy as jnp
from jax import lax
from jax.experimental import pallas as pl
from jax.experimental.pallas import tpu as pltpu
from jax.sharding import PartitionSpec as P

D = 5120
QH = 40
KVH = 8
HD = 128


BETA_ONE = 0.9
BETA_TWO = 0.999
FIRST_CORR = 0.9999734386011124
SECOND_CORR = 0.09520785288629041
LEARN_RATE = 0.003
EPSILON = 1e-08
ROPE_BASE = 1000000.0
NEG_FILL = -1e30


def rotate(new_keys, lengths):
    positions = (lengths[:, None] + jnp.arange(new_keys.shape[1], dtype=jnp.int32)[None, :]).astype(
        jnp.float32
    )
    half_dim = new_keys.shape[-1] // 2
    inverse = jnp.exp(
        -math.log(ROPE_BASE) * 2.0 * jnp.arange(half_dim, dtype=jnp.float32) / new_keys.shape[-1]
    )
    angles = positions[:, :, None] * inverse[None, None, :]
    cosine_part = jnp.concatenate([jnp.cos(angles), jnp.cos(angles)], -1)[:, :, None, :]
    sine_part = jnp.concatenate([jnp.sin(angles), jnp.sin(angles)], -1)[:, :, None, :]
    rotated = jnp.concatenate([-new_keys[..., half_dim:], new_keys[..., :half_dim]], -1)
    return new_keys * cosine_part + rotated * sine_part


def body(
    grad_parts,
    master,
    moment_one,
    moment_two,
    hidden_in,
    queries,
    cache_keys,
    cache_values,
    cache_lengths,
):
    col_width = master.shape[1]
    grad_sum = lax.psum_scatter(grad_parts[0], "tp", scatter_dimension=1, tiled=True)
    squares = lax.psum(jnp.sum(grad_sum * grad_sum), ("grp", "rep", "tp"))
    norm_limit = math.sqrt(D * 2 * KVH * HD)
    clipped = grad_sum * jnp.minimum(1.0, norm_limit / jnp.sqrt(squares))
    new_moment_one = BETA_ONE * moment_one + (1.0 - BETA_ONE) * clipped
    new_moment_two = BETA_TWO * moment_two + (1.0 - BETA_TWO) * clipped * clipped
    update = new_moment_one / FIRST_CORR / (jnp.sqrt(new_moment_two / SECOND_CORR) + EPSILON)
    weights = (master - LEARN_RATE * update).astype(jnp.bfloat16)
    row_count, step_count, model_width = hidden_in.shape
    token_count = row_count * step_count
    flat_inputs = hidden_in.reshape(token_count, model_width)
    sliced = lax.all_to_all(
        lax.all_to_all(flat_inputs, "grp", split_axis=1, concat_axis=0, tiled=True),
        "rep",
        split_axis=1,
        concat_axis=0,
        tiled=True,
    )
    group_count = lax.axis_size("grp")
    replica_count = lax.axis_size("rep")
    ordered = sliced.reshape(replica_count, group_count, token_count, weights.shape[0])
    ordered = jnp.swapaxes(ordered, 0, 1).reshape(
        group_count * replica_count * token_count, weights.shape[0]
    )
    projected = lax.psum_scatter(
        jnp.dot(ordered, weights, preferred_element_type=jnp.float32),
        ("grp", "rep"),
        scatter_dimension=0,
        tiled=True,
    )
    heads_here = col_width // (2 * HD)
    projected = projected.reshape(row_count, step_count, heads_here, 2, HD)
    new_keys = rotate(projected[:, :, :, 0, :], cache_lengths).astype(jnp.bfloat16)
    new_values = projected[:, :, :, 1, :].astype(jnp.bfloat16)
    new_entries = jnp.stack([new_keys, new_values], 3).reshape(row_count, step_count, col_width)
    groups = QH // KVH
    slots = cache_keys.shape[1]
    query_heads = queries.reshape(row_count, step_count, heads_here, groups, HD)
    old_k = cache_keys.reshape(row_count, slots, heads_here, HD)
    old_v = cache_values.reshape(row_count, slots, heads_here, HD)
    scaling = 1.0 / math.sqrt(HD)
    old_scores = (
        jnp.einsum("rsagd,rjad->rsagj", query_heads, old_k, preferred_element_type=jnp.float32)
        * scaling
    )
    valid_slots = jnp.arange(slots, dtype=jnp.int32)[None, :] < cache_lengths[:, None]
    old_scores = jnp.where(valid_slots[:, None, None, None, :], old_scores, NEG_FILL)
    new_scores = (
        jnp.einsum("rsagd,rtad->rsagt", query_heads, new_keys, preferred_element_type=jnp.float32)
        * scaling
    )
    causal = jnp.arange(step_count)[:, None] >= jnp.arange(step_count)[None, :]
    new_scores = jnp.where(causal[None, :, None, None, :], new_scores, NEG_FILL)
    scores = jnp.concatenate([old_scores, new_scores], -1)
    row_max = jnp.max(scores, -1, keepdims=True)
    exp_scores = jnp.exp(scores - row_max)
    probs = (exp_scores / jnp.sum(exp_scores, -1, keepdims=True)).astype(jnp.bfloat16)
    output = jnp.einsum(
        "rsagj,rjad->rsagd", probs[..., :slots], old_v, preferred_element_type=jnp.float32
    )
    output = output + jnp.einsum(
        "rsagt,rtad->rsagd", probs[..., slots:], new_values, preferred_element_type=jnp.float32
    )
    attended = output.reshape(row_count, step_count, heads_here * groups * HD).astype(jnp.bfloat16)
    return (new_moment_one, new_moment_two, new_entries, attended)


MESH = pl.DeviceIdType.MESH
PAD = 32
BLOCK = 128
EARLY = 2


def chunk_plan(rows):
    sizes = [32, 64]
    left = rows - sum(sizes) - 32
    while left > 0:
        sizes.append(min(96, left))
        left -= sizes[-1]
    sizes.append(32)
    return [(sum(sizes[:i]), n) for i, n in enumerate(sizes)]


def fused_kernel(
    sizes,
    lengths_ref,
    hidden_ref,
    queries_ref,
    grad_ref,
    master_ref,
    one_ref,
    two_ref,
    keys_ref,
    values_ref,
    one_out,
    two_out,
    proj_out,
    cos_out,
    sin_out,
    query_f,
    old_max,
    old_sum,
    old_out,
    lengths_s,
    queries_v,
    mate_src,
    fwd_in,
    fwd_send,
    sum_far,
    sum_in,
    grad_total,
    state_v,
    cache_v,
    hidden_in_v,
    hidden_f,
    hidden_b,
    weights_v,
    squares_send,
    squares_all,
    proj_own,
    proj_send,
    proj_recv,
    fwd_sem,
    far_recv_sem,
    proj_recv_sem,
    cache_sem,
    sum_sem,
    early_sem,
    mate_send_sem,
    far_send_sem,
    hid_send_sem,
    hid_recv_sem,
    sq_send_sem,
    sq_recv_sem,
    proj_send_sem,
    load_sem,
    length_sem,
    query_sem,
    own_sem,
    round_sem,
):
    ngrp, nrep, ntp = sizes
    ngroup = ngrp * nrep
    ndev = ngroup * ntp
    rows, cols = master_ref.shape
    nrow, nstep, width = hidden_ref.shape
    tokens = nrow * nstep
    slots = keys_ref.shape[1]
    heads = cols // (2 * HD)
    groups = QH // KVH
    plan = chunk_plan(rows)
    nchunk = len(plan)
    nblock = cols // BLOCK
    scaling = 1.0 / math.sqrt(HD)

    g = lax.axis_index("grp")
    r = lax.axis_index("rep")
    t = lax.axis_index("tp")
    p = g * nrep + r
    y = t // 2
    c = t % 2
    mate = y * 2 + (1 - c)
    far = (1 - y) * 2 + c
    far_mate = (1 - y) * 2 + (1 - c)

    def toggles(v, size):
        return [(1 << b) * (1 - 2 * lax.rem(lax.div(v, 1 << b), 2)) for b in range(size.bit_length() - 1)]

    flips = {"grp": toggles(g, ngrp), "rep": toggles(r, nrep), "tp": toggles(t, ntp)}
    base = {"grp": g, "rep": r, "tp": t}

    def peer(**bits):
        return {
            name: base[name] + sum(d for b, d in enumerate(flips[name]) if bits.get(name, 0) >> b & 1)
            for name in base
        }

    def group_bits(k):
        return {"grp": k // nrep, "rep": k % nrep}

    def group_peer(k):
        return peer(**group_bits(k))

    def flat_bits(k):
        return {"tp": k % ntp, **group_bits(k // ntp)}

    def hops(k):
        bits = flat_bits(k)
        return bits["grp"] + bits["rep"] + bits["tp"] // 2 + 0.3 * (bits["tp"] % 2)

    flat_order = sorted(range(1, ndev), key=hops, reverse=True)
    group_order = sorted(range(1, ngroup), key=lambda k: hops(k * ntp), reverse=True)

    barrier = pltpu.get_barrier_semaphore()
    bits = ndev.bit_length() - 1

    def across(b):
        return peer(**flat_bits(1 << b))

    for b in range(bits):
        pl.semaphore_signal(barrier, inc=1, device_id=across(b), device_id_type=MESH)

    def block(start, n, owner):
        return grad_ref.at[0, pl.ds(start, n), pl.ds(pl.multiple_of(owner * cols, cols), cols)]

    def drain(ref, sem):
        pltpu.make_async_copy(ref, ref, sem).wait()

    early = sum(n for _, n in plan[:EARLY])
    early_copy = pltpu.make_async_copy(block(0, early, far_mate), mate_src, early_sem)
    early_copy.start()

    def own_copy(i):
        start, n = plan[i]
        return pltpu.make_async_copy(block(start, n, far), fwd_in.at[pl.ds(2 * start, n)], fwd_sem.at[i])

    def mate_copy(i):
        start, n = plan[i]
        return pltpu.make_async_remote_copy(
            src_ref=mate_src.at[pl.ds(start, n)] if i < EARLY else block(start, n, far_mate),
            dst_ref=fwd_in.at[pl.ds(2 * start + n, n)],
            send_sem=mate_send_sem,
            recv_sem=fwd_sem.at[i],
            device_id=peer(tp=1),
            device_id_type=MESH,
        )

    def far_copy(i):
        start, n = plan[i]
        return pltpu.make_async_remote_copy(
            src_ref=fwd_send.at[pl.ds(start, n)],
            dst_ref=sum_far.at[pl.ds(start, n)],
            send_sem=far_send_sem,
            recv_sem=far_recv_sem.at[i],
            device_id=peer(tp=2),
            device_id_type=MESH,
        )

    def hid_copy(k):
        to = group_peer(k)
        q = to["grp"] * nrep + to["rep"]
        return pltpu.make_async_remote_copy(
            src_ref=hidden_ref.at[:, :, pl.ds(pl.multiple_of(q * rows, 128), rows)],
            dst_ref=hidden_in_v.at[k],
            send_sem=hid_send_sem,
            recv_sem=hid_recv_sem,
            device_id=to,
            device_id_type=MESH,
        )

    def sq_copy(k):
        return pltpu.make_async_remote_copy(
            src_ref=squares_send,
            dst_ref=squares_all.at[k],
            send_sem=sq_send_sem,
            recv_sem=sq_recv_sem,
            device_id=peer(**flat_bits(k)),
            device_id_type=MESH,
        )

    def proj_copy(j, k):
        return pltpu.make_async_remote_copy(
            src_ref=proj_send.at[j, k - 1],
            dst_ref=proj_recv.at[j, k - 1],
            send_sem=proj_send_sem,
            recv_sem=proj_recv_sem.at[j],
            device_id=group_peer(k),
            device_id_type=MESH,
        )

    for i in range(nchunk):
        own_copy(i).start()
    length_copy = pltpu.make_async_copy(lengths_ref, lengths_s, length_sem)
    query_copy = pltpu.make_async_copy(queries_ref, queries_v, query_sem)
    own_hidden = pltpu.make_async_copy(
        hidden_ref.at[:, :, pl.ds(pl.multiple_of(p * rows, 128), rows)], hidden_in_v.at[0], own_sem
    )
    for copy in (length_copy, query_copy, own_hidden):
        copy.start()

    early_copy.wait()
    pl.semaphore_wait(barrier, bits)

    for i in range(nchunk):
        mate_copy(i).start()
    pltpu.make_async_remote_copy(
        src_ref=block(0, rows, mate),
        dst_ref=sum_in.at[1],
        send_sem=mate_send_sem,
        recv_sem=sum_sem,
        device_id=peer(tp=1),
        device_id_type=MESH,
    ).start()
    for i in range(nrow):
        pltpu.make_async_copy(keys_ref.at[i], cache_v.at[i, 0], cache_sem.at[i]).start()
        pltpu.make_async_copy(values_ref.at[i], cache_v.at[i, 1], cache_sem.at[i]).start()
    pltpu.make_async_copy(block(0, rows, t), sum_in.at[0], sum_sem).start()
    for i, src in enumerate((one_ref, two_ref, master_ref)):
        pltpu.make_async_copy(src, state_v.at[i], load_sem).start()

    def forward(i):
        start, n = plan[i]
        drain(fwd_in.at[pl.ds(2 * start, 2 * n)], fwd_sem.at[i])
        fwd_send[start : start + n, :] = (
            fwd_in[2 * start : 2 * start + n, :] + fwd_in[2 * start + n : 2 * start + 2 * n, :]
        ).astype(jnp.bfloat16)
        far_copy(i).start()

    for b in range(bits):
        pl.semaphore_signal(round_sem.at[b], inc=1, device_id=across(b), device_id_type=MESH)
        for i in range(b * nchunk // bits, (b + 1) * nchunk // bits):
            forward(i)
        pl.semaphore_wait(round_sem.at[b], 1)
    for k in group_order:
        hid_copy(k).start()

    for copy in (length_copy, query_copy):
        copy.wait()
    query_f[...] = jnp.zeros_like(query_f)
    for i in range(nrow):
        row_q = queries_v[i].astype(jnp.float32)
        for a in range(heads):
            for j in range(groups):
                n = a * groups + j
                query_f[a, i * PAD + j * nstep : i * PAD + (j + 1) * nstep, :] = row_q[:, n * HD : (n + 1) * HD]

    slot = lax.broadcasted_iota(jnp.int32, (PAD, slots), 1)
    for i in range(nrow):
        drain(cache_v.at[i], cache_sem.at[i])
        valid = slot < lengths_s[i]
        for a in range(heads):
            q = query_f[a, i * PAD : (i + 1) * PAD, :].astype(jnp.bfloat16)
            scores = lax.dot_general(
                q,
                cache_v[i, 0, :, a * HD : (a + 1) * HD],
                (((1,), (1,)), ((), ())),
                preferred_element_type=jnp.float32,
            )
            scores = jnp.where(valid, scores * scaling, NEG_FILL)
            top = jnp.max(scores, -1, keepdims=True)
            e = jnp.exp(scores - top)
            here = slice(i * PAD, (i + 1) * PAD)
            old_max[a, here, :] = jnp.broadcast_to(top, (PAD, HD))
            old_sum[a, here, :] = jnp.broadcast_to(jnp.sum(e, -1, keepdims=True), (PAD, HD))
            old_out[a, here, :] = jnp.dot(
                e.astype(jnp.bfloat16), cache_v[i, 1, :, a * HD : (a + 1) * HD], preferred_element_type=jnp.float32
            )

    token = lax.broadcasted_iota(jnp.int32, (tokens, HD), 0)
    lane = lax.broadcasted_iota(jnp.int32, (tokens, HD), 1)
    position = lax.rem(token, nstep)
    for i in range(nrow):
        position = position + jnp.where(token // nstep == i, lengths_s[i], 0)
    pair = lax.rem(lane, HD // 2).astype(jnp.float32)
    angle = position.astype(jnp.float32) * jnp.exp(-math.log(ROPE_BASE) * 2.0 * pair / HD)
    cos_out[...] = jnp.cos(angle)
    sin_out[...] = jnp.where(lane < HD // 2, -jnp.sin(angle), jnp.sin(angle))

    drain(state_v, load_sem)

    def prescale(i, carry):
        here = pl.ds(pl.multiple_of(i * 64, 64), 64)
        state_v[0, here, :] = BETA_ONE * state_v[0, here, :]
        state_v[1, here, :] = BETA_TWO * state_v[1, here, :]
        return carry

    lax.fori_loop(0, rows // 64, prescale, 0)

    own_hidden.wait()
    drain(hidden_in_v.at[pl.ds(1, ngroup - 1)], hid_recv_sem)
    for k in range(ngroup):
        own = hidden_in_v[k]
        for i in range(nrow):
            at = k * tokens + i * nstep
            hidden_f[at : at + nstep, :] = own[i].astype(jnp.float32)
    hidden_b[...] = hidden_f[...].astype(jnp.bfloat16)

    drain(sum_in, sum_sem)
    acc = jnp.zeros((8, cols), jnp.float32)
    for i, (start, n) in enumerate(plan):
        here = slice(start, start + n)
        drain(sum_far.at[pl.ds(start, n)], far_recv_sem.at[i])
        s = sum_in[0, here, :] + sum_in[1, here, :] + sum_far[here, :].astype(jnp.float32)
        grad_total[here, :] = s
        acc = acc + jnp.sum((s * s).reshape(n // 8, 8, cols), axis=0)
    mine = jnp.sum(sum(acc[:, j * 128 : (j + 1) * 128] for j in range(cols // 128)), axis=0, keepdims=True)
    squares_send[...] = mine
    for k in flat_order:
        sq_copy(k).start()
    squares_all[0] = mine
    drain(fwd_in, mate_send_sem)
    drain(fwd_send, far_send_sem)
    drain(hidden_in_v.at[pl.ds(1, ngroup - 1)], hid_send_sem)
    drain(squares_all.at[pl.ds(1, ndev - 1)], sq_recv_sem)
    squares = jnp.sum(jnp.sum(squares_all[...], axis=0), axis=1, keepdims=True)
    norm_limit = math.sqrt(D * 2 * KVH * HD)
    factor = jnp.minimum(1.0, norm_limit / jnp.sqrt(jnp.broadcast_to(squares, (1, BLOCK))))
    factor_one = (1.0 - BETA_ONE) * factor
    factor_two = (1.0 - BETA_TWO) * factor * factor

    for j in range(nblock):
        lanes = slice(j * BLOCK, (j + 1) * BLOCK)
        s = grad_total[:, lanes]
        one = state_v[0, :, lanes] + factor_one * s
        two = state_v[1, :, lanes] + factor_two * (s * s)
        one_out[:, lanes] = one
        two_out[:, lanes] = two
        v = two * (1.0 / SECOND_CORR)
        update = (one * (LEARN_RATE / FIRST_CORR)) / (v * lax.rsqrt(v) + EPSILON)
        weights_v[:, lanes] = (state_v[2, :, lanes] - update).astype(jnp.bfloat16)
        partial = jnp.dot(hidden_b[...], weights_v[:, lanes], preferred_element_type=jnp.float32)
        for k in group_order:
            proj_send[j, k - 1] = partial[k * tokens : (k + 1) * tokens].astype(jnp.bfloat16)
        for k in group_order:
            proj_copy(j, k).start()
        proj_own[:, lanes] = partial[0:tokens]

    drain(squares_all.at[pl.ds(1, ndev - 1)], sq_send_sem)
    for j in range(nblock):
        lanes = slice(j * BLOCK, (j + 1) * BLOCK)
        projected = proj_own[:, lanes]
        drain(proj_recv.at[j], proj_recv_sem.at[j])
        for k in range(1, ngroup):
            projected = projected + proj_recv[j, k - 1].astype(jnp.float32)
        proj_out[:, lanes] = projected
    drain(proj_send, proj_send_sem)


def finish_kernel(
    one_ref,
    two_ref,
    proj_ref,
    cos_ref,
    sin_ref,
    query_ref,
    max_ref,
    sum_ref,
    old_ref,
    one_out,
    two_out,
    entries_out,
    attended_out,
    heads_v,
    out_sem,
):
    outs = [
        pltpu.make_async_copy(one_ref, one_out, out_sem.at[0]),
        pltpu.make_async_copy(two_ref, two_out, out_sem.at[1]),
    ]
    for copy in outs:
        copy.start()
    nrow, nstep, cols = entries_out.shape
    tokens = nrow * nstep
    heads = cols // (2 * HD)
    groups = QH // KVH
    scaling = 1.0 / math.sqrt(HD)
    qi = lax.broadcasted_iota(jnp.int32, (nrow * PAD, tokens), 0)
    kj = lax.broadcasted_iota(jnp.int32, (nrow * PAD, tokens), 1)
    seen = (qi // PAD == kj // nstep) & (qi % nstep >= kj % nstep)
    for a in range(heads):
        k = proj_ref[:, 2 * a * HD : (2 * a + 1) * HD]
        k = k * cos_ref[...] + pltpu.roll(k, HD // 2, 1) * sin_ref[...]
        v = proj_ref[:, (2 * a + 1) * HD : (2 * a + 2) * HD]
        new_k = k.astype(jnp.bfloat16)
        new_v = v.astype(jnp.bfloat16)
        for i in range(nrow):
            rows_i = slice(i * nstep, (i + 1) * nstep)
            entries_out[i, :, 2 * a * HD : (2 * a + 1) * HD] = k[rows_i].astype(jnp.bfloat16)
            entries_out[i, :, (2 * a + 1) * HD : (2 * a + 2) * HD] = v[rows_i].astype(jnp.bfloat16)
        scores = lax.dot_general(
            query_ref[a].astype(jnp.bfloat16), new_k, (((1,), (1,)), ((), ())), preferred_element_type=jnp.float32
        )
        scores = jnp.where(seen, scores * scaling, NEG_FILL)
        before = max_ref[a][:, 0:1]
        top = jnp.maximum(before, jnp.max(scores, -1, keepdims=True))
        alpha = jnp.exp(before - top)
        e = jnp.exp(scores - top)
        whole = sum_ref[a][:, 0:1] * alpha + jnp.sum(e, -1, keepdims=True)
        o = old_ref[a] * alpha + jnp.dot(e.astype(jnp.bfloat16), new_v, preferred_element_type=jnp.float32)
        heads_v[a] = o / whole
        for i in range(nrow):
            for j in range(groups):
                n = a * groups + j
                at = i * PAD + j * nstep
                attended_out[i, :, n * HD : (n + 1) * HD] = heads_v[a, at : at + nstep, :].astype(jnp.bfloat16)
    for copy in outs:
        copy.wait()


def fused_body(
    sizes,
    grad_parts,
    master,
    moment_one,
    moment_two,
    hidden_in,
    queries,
    cache_keys,
    cache_values,
    cache_lengths,
):
    ngrp, nrep, ntp = sizes
    ngroup = ngrp * nrep
    ndev = ngroup * ntp
    rows, cols = master.shape
    nrow, nstep, width = hidden_in.shape
    tokens = nrow * nstep
    heads = cols // (2 * HD)
    plan = chunk_plan(rows)
    f32, bf16 = jnp.float32, jnp.bfloat16
    vm = pltpu.VMEM
    dma = pltpu.SemaphoreType.DMA
    vmem = pl.BlockSpec(memory_space=pltpu.VMEM)
    hbm = pl.BlockSpec(memory_space=pltpu.HBM)
    per_head = vm((heads, nrow * PAD, HD), f32)
    moment = vm((rows, cols), f32)
    table = vm((tokens, HD), f32)
    middle = pl.pallas_call(
        functools.partial(fused_kernel, sizes),
        out_shape=(moment, moment, vm((tokens, cols), f32), table, table) + (per_head,) * 4,
        in_specs=[hbm] * 9,
        out_specs=(vmem,) * 9,
        scratch_shapes=[
            pltpu.SMEM((nrow,), jnp.int32),
            vm(queries.shape, bf16),
            vm((sum(n for _, n in plan[:EARLY]), cols), f32),
            vm((2 * rows, cols), f32),
            vm((rows, cols), bf16),
            vm((rows, cols), bf16),
            vm((2, rows, cols), f32),
            vm((rows, cols), f32),
            vm((3, rows, cols), f32),
            vm((nrow, 2) + cache_keys.shape[1:], bf16),
            vm((ngroup, nrow, nstep, rows), bf16),
            vm((ngroup * tokens, rows), f32),
            vm((ngroup * tokens, rows), bf16),
            vm((rows, cols), bf16),
            vm((1, 128), f32),
            vm((ndev, 1, 128), f32),
            vm((tokens, cols), f32),
            vm((cols // BLOCK, ngroup - 1, tokens, BLOCK), bf16),
            vm((cols // BLOCK, ngroup - 1, tokens, BLOCK), bf16),
            dma((len(plan),)),
            dma((len(plan),)),
            dma((cols // BLOCK,)),
            dma((nrow,)),
        ]
        + [pltpu.SemaphoreType.DMA] * 13
        + [pltpu.SemaphoreType.REGULAR((ndev.bit_length() - 1,))],
        compiler_params=pltpu.CompilerParams(
            collective_id=0, has_side_effects=True, vmem_limit_bytes=60 * 1024 * 1024 + 320 * 1024
        ),
    )(cache_lengths, hidden_in, queries, grad_parts, master, moment_one, moment_two, cache_keys, cache_values)
    return pl.pallas_call(
        finish_kernel,
        out_shape=(
            jax.ShapeDtypeStruct((rows, cols), f32),
            jax.ShapeDtypeStruct((rows, cols), f32),
            jax.ShapeDtypeStruct((nrow, nstep, cols), bf16),
            jax.ShapeDtypeStruct(queries.shape, bf16),
        ),
        in_specs=[vmem] * 9,
        out_specs=(hbm, hbm, vmem, vmem),
        scratch_shapes=[vm((heads, nrow * PAD, HD), f32), dma((2,))],
        compiler_params=pltpu.CompilerParams(vmem_limit_bytes=8 * 1024 * 1024),
    )(*middle)


def solution(mesh):
    sizes = (mesh.shape["grp"], mesh.shape["rep"], mesh.shape["tp"])
    fits = sizes[2] == 4 and D % (sizes[0] * sizes[1] * 128) == 0 and KVH % sizes[2] == 0
    fits = fits and (sizes[0] * sizes[1]) & (sizes[0] * sizes[1] - 1) == 0
    placed = (
        P("tp", ("grp", "rep"), None),
        P(("grp", "rep"), "tp"),
        P(("grp", "rep"), "tp"),
        P(("grp", "rep"), "tp"),
        P(("grp", "rep"), None, None),
        P(("grp", "rep"), None, "tp"),
        P(("grp", "rep"), None, "tp"),
        P(("grp", "rep"), None, "tp"),
        P(("grp", "rep")),
    )
    return jax.shard_map(
        functools.partial(fused_body, sizes) if fits else body,
        mesh=mesh,
        in_specs=placed,
        out_specs=(
            P(("grp", "rep"), "tp"),
            P(("grp", "rep"), "tp"),
            P(("grp", "rep"), None, "tp"),
            P(("grp", "rep"), None, "tp"),
        ),
        check_vma=False,
    )
```

```python
import functools
import math

import jax
import jax.numpy as jnp
from jax import lax
from jax.experimental import pallas as pl
from jax.experimental.pallas import tpu as pltpu
from jax.sharding import PartitionSpec as P

D = 5120
QH = 40
KVH = 8
HD = 128


BETA_ONE = 0.9
BETA_TWO = 0.999
FIRST_CORR = 0.9999734386011124
SECOND_CORR = 0.09520785288629041
LEARN_RATE = 0.003
EPSILON = 1e-08
ROPE_BASE = 1000000.0
NEG_FILL = -1e30


def rotate(new_keys, lengths):
    positions = (lengths[:, None] + jnp.arange(new_keys.shape[1], dtype=jnp.int32)[None, :]).astype(
        jnp.float32
    )
    half_dim = new_keys.shape[-1] // 2
    inverse = jnp.exp(
        -math.log(ROPE_BASE) * 2.0 * jnp.arange(half_dim, dtype=jnp.float32) / new_keys.shape[-1]
    )
    angles = positions[:, :, None] * inverse[None, None, :]
    cosine_part = jnp.concatenate([jnp.cos(angles), jnp.cos(angles)], -1)[:, :, None, :]
    sine_part = jnp.concatenate([jnp.sin(angles), jnp.sin(angles)], -1)[:, :, None, :]
    rotated = jnp.concatenate([-new_keys[..., half_dim:], new_keys[..., :half_dim]], -1)
    return new_keys * cosine_part + rotated * sine_part


def body(
    grad_parts,
    master,
    moment_one,
    moment_two,
    hidden_in,
    queries,
    cache_keys,
    cache_values,
    cache_lengths,
):
    col_width = master.shape[1]
    grad_sum = lax.psum_scatter(grad_parts[0], "tp", scatter_dimension=1, tiled=True)
    squares = lax.psum(jnp.sum(grad_sum * grad_sum), ("grp", "rep", "tp"))
    norm_limit = math.sqrt(D * 2 * KVH * HD)
    clipped = grad_sum * jnp.minimum(1.0, norm_limit / jnp.sqrt(squares))
    new_moment_one = BETA_ONE * moment_one + (1.0 - BETA_ONE) * clipped
    new_moment_two = BETA_TWO * moment_two + (1.0 - BETA_TWO) * clipped * clipped
    update = new_moment_one / FIRST_CORR / (jnp.sqrt(new_moment_two / SECOND_CORR) + EPSILON)
    weights = (master - LEARN_RATE * update).astype(jnp.bfloat16)
    row_count, step_count, model_width = hidden_in.shape
    token_count = row_count * step_count
    flat_inputs = hidden_in.reshape(token_count, model_width)
    sliced = lax.all_to_all(
        lax.all_to_all(flat_inputs, "grp", split_axis=1, concat_axis=0, tiled=True),
        "rep",
        split_axis=1,
        concat_axis=0,
        tiled=True,
    )
    group_count = lax.axis_size("grp")
    replica_count = lax.axis_size("rep")
    ordered = sliced.reshape(replica_count, group_count, token_count, weights.shape[0])
    ordered = jnp.swapaxes(ordered, 0, 1).reshape(
        group_count * replica_count * token_count, weights.shape[0]
    )
    projected = lax.psum_scatter(
        jnp.dot(ordered, weights, preferred_element_type=jnp.float32),
        ("grp", "rep"),
        scatter_dimension=0,
        tiled=True,
    )
    heads_here = col_width // (2 * HD)
    projected = projected.reshape(row_count, step_count, heads_here, 2, HD)
    new_keys = rotate(projected[:, :, :, 0, :], cache_lengths).astype(jnp.bfloat16)
    new_values = projected[:, :, :, 1, :].astype(jnp.bfloat16)
    new_entries = jnp.stack([new_keys, new_values], 3).reshape(row_count, step_count, col_width)
    groups = QH // KVH
    slots = cache_keys.shape[1]
    query_heads = queries.reshape(row_count, step_count, heads_here, groups, HD)
    old_k = cache_keys.reshape(row_count, slots, heads_here, HD)
    old_v = cache_values.reshape(row_count, slots, heads_here, HD)
    scaling = 1.0 / math.sqrt(HD)
    old_scores = (
        jnp.einsum("rsagd,rjad->rsagj", query_heads, old_k, preferred_element_type=jnp.float32)
        * scaling
    )
    valid_slots = jnp.arange(slots, dtype=jnp.int32)[None, :] < cache_lengths[:, None]
    old_scores = jnp.where(valid_slots[:, None, None, None, :], old_scores, NEG_FILL)
    new_scores = (
        jnp.einsum("rsagd,rtad->rsagt", query_heads, new_keys, preferred_element_type=jnp.float32)
        * scaling
    )
    causal = jnp.arange(step_count)[:, None] >= jnp.arange(step_count)[None, :]
    new_scores = jnp.where(causal[None, :, None, None, :], new_scores, NEG_FILL)
    scores = jnp.concatenate([old_scores, new_scores], -1)
    row_max = jnp.max(scores, -1, keepdims=True)
    exp_scores = jnp.exp(scores - row_max)
    probs = (exp_scores / jnp.sum(exp_scores, -1, keepdims=True)).astype(jnp.bfloat16)
    output = jnp.einsum(
        "rsagj,rjad->rsagd", probs[..., :slots], old_v, preferred_element_type=jnp.float32
    )
    output = output + jnp.einsum(
        "rsagt,rtad->rsagd", probs[..., slots:], new_values, preferred_element_type=jnp.float32
    )
    attended = output.reshape(row_count, step_count, heads_here * groups * HD).astype(jnp.bfloat16)
    return (new_moment_one, new_moment_two, new_entries, attended)


MESH = pl.DeviceIdType.MESH
PAD = 32
BLOCK = 256
DIRECT = 64
STEP_SIZE = LEARN_RATE / FIRST_CORR * math.sqrt(SECOND_CORR)
STEP_EPSILON = EPSILON * math.sqrt(SECOND_CORR)


def chunk_plan(rows):
    sizes = [DIRECT // 2, DIRECT // 2, DIRECT // 2, DIRECT // 2, 64]
    left = rows - sum(sizes) - 32
    while left > 0:
        sizes.append(min(96, left))
        left -= sizes[-1]
    sizes.append(32)
    return [(sum(sizes[:i]), n) for i, n in enumerate(sizes)]


def fused_kernel(
    sizes,
    lengths_ref,
    hidden_ref,
    queries_ref,
    grad_ref,
    master_ref,
    one_ref,
    two_ref,
    keys_ref,
    values_ref,
    one_out,
    two_out,
    proj_out,
    cos_out,
    sin_out,
    query_f,
    old_max,
    old_sum,
    old_out,
    lengths_s,
    queries_v,
    mate_src,
    direct_src,
    direct_send,
    direct_in,
    fwd_in,
    fwd_send,
    sum_far,
    sum_in,
    grad_total,
    grad_square,
    step_v,
    state_v,
    cache_v,
    hidden_in_v,
    hidden_f,
    hidden_b,
    squares_send,
    squares_all,
    proj_own,
    proj_send,
    proj_recv,
    fwd_sem,
    far_recv_sem,
    proj_recv_sem,
    sum_sem,
    direct_recv_sem,
    hid_recv_sem,
    sq_recv_sem,
    round_sem,
    cache_sem,
    early_sem,
    first_sem,
    direct_send_sem,
    mate_send_sem,
    far_send_sem,
    hid_send_sem,
    sq_send_sem,
    proj_send_sem,
    load_sem,
    length_sem,
    query_sem,
    own_sem,
):
    ngrp, nrep, ntp = sizes
    ngroup = ngrp * nrep
    ndev = ngroup * ntp
    rows, cols = master_ref.shape
    nrow, nstep, width = hidden_ref.shape
    tokens = nrow * nstep
    slots = keys_ref.shape[1]
    heads = cols // (2 * HD)
    groups = QH // KVH
    plan = chunk_plan(rows)
    nchunk = len(plan)
    nblock = cols // BLOCK
    scaling = 1.0 / math.sqrt(HD)

    g = lax.axis_index("grp")
    r = lax.axis_index("rep")
    t = lax.axis_index("tp")
    p = g * nrep + r
    y = t // 2
    c = t % 2
    mate = y * 2 + (1 - c)
    far = (1 - y) * 2 + c
    far_mate = (1 - y) * 2 + (1 - c)

    def toggles(v, size):
        return [(1 << b) * (1 - 2 * lax.rem(lax.div(v, 1 << b), 2)) for b in range(size.bit_length() - 1)]

    flips = {"grp": toggles(g, ngrp), "rep": toggles(r, nrep), "tp": toggles(t, ntp)}
    base = {"grp": g, "rep": r, "tp": t}

    def peer(**bits):
        return {
            name: base[name] + sum(d for b, d in enumerate(flips[name]) if bits.get(name, 0) >> b & 1)
            for name in base
        }

    def group_bits(k):
        return {"grp": k // nrep, "rep": k % nrep}

    def group_peer(k):
        return peer(**group_bits(k))

    def flat_bits(k):
        return {"tp": k % ntp, **group_bits(k // ntp)}

    def hops(k):
        bits = flat_bits(k)
        return bits["grp"] + bits["rep"] + bits["tp"] // 2 + 0.3 * (bits["tp"] % 2)

    flat_order = sorted(range(1, ndev), key=hops, reverse=True)
    group_order = sorted(range(1, ngroup), key=lambda k: hops(k * ntp), reverse=True)

    barrier = pltpu.get_barrier_semaphore()
    bits = ndev.bit_length() - 1

    def across(b):
        return peer(**flat_bits(1 << b))

    for b in range(bits):
        pl.semaphore_signal(barrier, inc=1, device_id=across(b), device_id_type=MESH)
    pl.semaphore_signal(barrier, inc=1, device_id=peer(tp=3), device_id_type=MESH)

    def block(start, n, owner):
        return grad_ref.at[0, pl.ds(start, n), pl.ds(pl.multiple_of(owner * cols, cols), cols)]

    def drain(ref, sem):
        pltpu.make_async_copy(ref, ref, sem).wait()

    target = (1 - y) * 2
    direct_copy = pltpu.make_async_copy(block(0, DIRECT, target), direct_src, first_sem)
    early_start = pl.multiple_of(c * DIRECT, DIRECT)
    early_copy = pltpu.make_async_copy(block(early_start, DIRECT, far_mate), mate_src, early_sem)
    early_copy.start()
    direct_copy.start()

    direct_put = pltpu.make_async_remote_copy(
        src_ref=direct_send,
        dst_ref=direct_in.at[c],
        send_sem=direct_send_sem,
        recv_sem=direct_recv_sem,
        device_id={**base, "tp": target},
        device_id_type=MESH,
    )

    def early_mate(i):
        half = DIRECT // 2
        return pltpu.make_async_remote_copy(
            src_ref=mate_src.at[pl.ds(i * half, half)],
            dst_ref=fwd_in.at[pl.ds(pl.multiple_of(2 * (early_start + i * half) + half, half), half)],
            send_sem=mate_send_sem,
            recv_sem=fwd_sem.at[2 * c + i],
            device_id=peer(tp=1),
            device_id_type=MESH,
        )

    def own_copy(i):
        start, n = plan[i]
        return pltpu.make_async_copy(block(start, n, far), fwd_in.at[pl.ds(2 * start, n)], fwd_sem.at[i])

    def mate_copy(i):
        start, n = plan[i]
        return pltpu.make_async_remote_copy(
            src_ref=block(start, n, far_mate),
            dst_ref=fwd_in.at[pl.ds(2 * start + n, n)],
            send_sem=mate_send_sem,
            recv_sem=fwd_sem.at[i],
            device_id=peer(tp=1),
            device_id_type=MESH,
        )

    def far_copy(i):
        start, n = plan[i]
        return pltpu.make_async_remote_copy(
            src_ref=fwd_send.at[pl.ds(start, n)],
            dst_ref=sum_far.at[pl.ds(start, n)],
            send_sem=far_send_sem,
            recv_sem=far_recv_sem.at[i],
            device_id=peer(tp=2),
            device_id_type=MESH,
        )

    def hid_copy(k):
        to = group_peer(k)
        q = to["grp"] * nrep + to["rep"]
        return pltpu.make_async_remote_copy(
            src_ref=hidden_ref.at[:, :, pl.ds(pl.multiple_of(q * rows, 128), rows)],
            dst_ref=hidden_in_v.at[k],
            send_sem=hid_send_sem,
            recv_sem=hid_recv_sem,
            device_id=to,
            device_id_type=MESH,
        )

    def sq_copy(k):
        return pltpu.make_async_remote_copy(
            src_ref=squares_send,
            dst_ref=squares_all.at[k],
            send_sem=sq_send_sem,
            recv_sem=sq_recv_sem,
            device_id=peer(**flat_bits(k)),
            device_id_type=MESH,
        )

    def proj_copy(j, k):
        return pltpu.make_async_remote_copy(
            src_ref=proj_send.at[j, k - 1],
            dst_ref=proj_recv.at[j, k - 1],
            send_sem=proj_send_sem,
            recv_sem=proj_recv_sem.at[j],
            device_id=group_peer(k),
            device_id_type=MESH,
        )

    length_copy = pltpu.make_async_copy(lengths_ref, lengths_s, length_sem)
    query_copy = pltpu.make_async_copy(queries_ref, queries_v, query_sem)
    own_hidden = pltpu.make_async_copy(
        hidden_ref.at[:, :, pl.ds(pl.multiple_of(p * rows, 128), rows)], hidden_in_v.at[0], own_sem
    )

    early_copy.wait()
    pl.semaphore_wait(barrier, bits + 1)

    early_mate(0).start()
    early_mate(1).start()
    direct_copy.wait()
    direct_send[...] = direct_src[...].astype(jnp.bfloat16)
    direct_put.start()

    @pl.when(c == 1)
    def _():
        own_copy(0).start()
        own_copy(1).start()

    for i in range(2, nchunk):
        own_copy(i).start()

    @pl.when(c == 0)
    def _():
        mate_copy(2).start()
        mate_copy(3).start()

    for i in range(4, nchunk):
        mate_copy(i).start()
    pltpu.make_async_remote_copy(
        src_ref=block(0, rows, mate),
        dst_ref=sum_in.at[1],
        send_sem=mate_send_sem,
        recv_sem=sum_sem,
        device_id=peer(tp=1),
        device_id_type=MESH,
    ).start()
    for copy in (length_copy, query_copy, own_hidden):
        copy.start()
    for i in range(nrow):
        pltpu.make_async_copy(keys_ref.at[i], cache_v.at[i, 0], cache_sem.at[i]).start()
        pltpu.make_async_copy(values_ref.at[i], cache_v.at[i, 1], cache_sem.at[i]).start()
    pltpu.make_async_copy(block(0, rows, t), sum_in.at[0], sum_sem).start()
    for i, src in enumerate((one_ref, two_ref, master_ref)):
        pltpu.make_async_copy(src, state_v.at[i], load_sem).start()

    def forward(i):
        start, n = plan[i]
        drain(fwd_in.at[pl.ds(2 * start, 2 * n)], fwd_sem.at[i])
        fwd_send[start : start + n, :] = (
            fwd_in[2 * start : 2 * start + n, :] + fwd_in[2 * start + n : 2 * start + 2 * n, :]
        ).astype(jnp.bfloat16)
        far_copy(i).start()

    for b in range(bits):
        pl.semaphore_signal(round_sem.at[b], inc=1, device_id=across(b), device_id_type=MESH)
        for i in range(b * nchunk // bits, (b + 1) * nchunk // bits):
            if i < 2:
                pl.when(c == 1)(functools.partial(forward, i))
            else:
                forward(i)
        pl.semaphore_wait(round_sem.at[b], 1)
    for k in group_order:
        hid_copy(k).start()

    for copy in (length_copy, query_copy):
        copy.wait()
    query_f[...] = jnp.zeros_like(query_f)
    for i in range(nrow):
        row_q = queries_v[i].astype(jnp.float32)
        for a in range(heads):
            for j in range(groups):
                n = a * groups + j
                query_f[a, i * PAD + j * nstep : i * PAD + (j + 1) * nstep, :] = row_q[:, n * HD : (n + 1) * HD]

    slot = lax.broadcasted_iota(jnp.int32, (PAD, slots), 1)
    for i in range(nrow):
        drain(cache_v.at[i], cache_sem.at[i])
        valid = slot < lengths_s[i]
        for a in range(heads):
            q = query_f[a, i * PAD : (i + 1) * PAD, :].astype(jnp.bfloat16)
            scores = lax.dot_general(
                q,
                cache_v[i, 0, :, a * HD : (a + 1) * HD],
                (((1,), (1,)), ((), ())),
                preferred_element_type=jnp.float32,
            )
            scores = jnp.where(valid, scores * scaling, NEG_FILL)
            top = jnp.max(scores, -1, keepdims=True)
            e = jnp.exp(scores - top)
            here = slice(i * PAD, (i + 1) * PAD)
            old_max[a, here, :] = jnp.broadcast_to(top, (PAD, HD))
            old_sum[a, here, :] = jnp.broadcast_to(jnp.sum(e, -1, keepdims=True), (PAD, HD))
            old_out[a, here, :] = jnp.dot(
                e.astype(jnp.bfloat16), cache_v[i, 1, :, a * HD : (a + 1) * HD], preferred_element_type=jnp.float32
            )

    token = lax.broadcasted_iota(jnp.int32, (tokens, HD), 0)
    lane = lax.broadcasted_iota(jnp.int32, (tokens, HD), 1)
    position = lax.rem(token, nstep)
    for i in range(nrow):
        position = position + jnp.where(token // nstep == i, lengths_s[i], 0)
    pair = lax.rem(lane, HD // 2).astype(jnp.float32)
    angle = position.astype(jnp.float32) * jnp.exp(-math.log(ROPE_BASE) * 2.0 * pair / HD)
    cos_out[...] = jnp.cos(angle)
    sin_out[...] = jnp.where(lane < HD // 2, -jnp.sin(angle), jnp.sin(angle))

    drain(state_v, load_sem)

    def prescale(i, carry):
        here = pl.ds(pl.multiple_of(i * 64, 64), 64)
        step_v[here, :] = (BETA_ONE * STEP_SIZE) * state_v[0, here, :]
        state_v[1, here, :] = BETA_TWO * state_v[1, here, :]
        return carry

    lax.fori_loop(0, rows // 64, prescale, 0)

    own_hidden.wait()
    drain(hidden_in_v.at[pl.ds(1, ngroup - 1)], hid_recv_sem)
    for k in range(ngroup):
        own = hidden_in_v[k]
        for i in range(nrow):
            at = k * tokens + i * nstep
            hidden_f[at : at + nstep, :] = own[i].astype(jnp.float32)
    hidden_b[...] = hidden_f[...].astype(jnp.bfloat16)

    drain(sum_in, sum_sem)

    @pl.when(c == 0)
    def _():
        drain(direct_in, direct_recv_sem)
        sum_in[0, :DIRECT, :] = (
            sum_in[0, :DIRECT, :] + direct_in[0].astype(jnp.float32) + direct_in[1].astype(jnp.float32)
        )
        sum_far[:DIRECT, :] = jnp.zeros((DIRECT, cols), jnp.bfloat16)

    @pl.when(c == 1)
    def _():
        for i in range(2):
            start, n = plan[i]
            drain(sum_far.at[pl.ds(start, n)], far_recv_sem.at[i])

    acc = jnp.zeros((8, cols), jnp.float32)
    for i, (start, n) in enumerate(plan):
        here = slice(start, start + n)
        if i > 1:
            drain(sum_far.at[pl.ds(start, n)], far_recv_sem.at[i])
        s = sum_in[0, here, :] + sum_in[1, here, :] + sum_far[here, :].astype(jnp.float32)
        grad_total[here, :] = s
        square = s * s
        grad_square[here, :] = square
        acc = acc + jnp.sum(square.reshape(n // 8, 8, cols), axis=0)
    mine = jnp.sum(sum(acc[:, j * 128 : (j + 1) * 128] for j in range(cols // 128)), axis=0, keepdims=True)
    squares_send[...] = mine
    for k in flat_order:
        sq_copy(k).start()
    squares_all[0] = mine
    drain(direct_send, direct_send_sem)

    @pl.when(c == 0)
    def _():
        drain(fwd_in, mate_send_sem)
        drain(fwd_send.at[pl.ds(DIRECT, rows - DIRECT)], far_send_sem)

    @pl.when(c == 1)
    def _():
        drain(fwd_in.at[pl.ds(DIRECT, 2 * rows - DIRECT)], mate_send_sem)
        drain(fwd_send, far_send_sem)

    drain(hidden_in_v.at[pl.ds(1, ngroup - 1)], hid_send_sem)
    drain(squares_all.at[pl.ds(1, ndev - 1)], sq_recv_sem)
    squares = jnp.sum(jnp.sum(squares_all[...], axis=0), axis=1, keepdims=True)
    norm_limit = math.sqrt(D * 2 * KVH * HD)
    factor = jnp.minimum(1.0, norm_limit / jnp.sqrt(jnp.broadcast_to(squares, (1, BLOCK))))
    factor_step = ((1.0 - BETA_ONE) * STEP_SIZE) * factor
    factor_two = (1.0 - BETA_TWO) * factor * factor

    def weights(lanes):
        step = step_v[:, lanes] + factor_step * grad_total[:, lanes]
        two = state_v[1, :, lanes] + factor_two * grad_square[:, lanes]
        return (state_v[2, :, lanes] - step / (two * lax.rsqrt(two) + STEP_EPSILON)).astype(jnp.bfloat16)

    for j in range(nblock):
        lanes = slice(j * BLOCK, (j + 1) * BLOCK)
        partial = jnp.dot(hidden_b[...], weights(lanes), preferred_element_type=jnp.float32)
        for k in group_order:
            proj_send[j, k - 1] = partial[k * tokens : (k + 1) * tokens].astype(jnp.bfloat16)
        for k in group_order:
            proj_copy(j, k).start()
        proj_own[:, lanes] = partial[0:tokens]

    factor_one = (1.0 - BETA_ONE) * factor
    for j in range(nblock):
        lanes = slice(j * BLOCK, (j + 1) * BLOCK)
        one_out[:, lanes] = BETA_ONE * state_v[0, :, lanes] + factor_one * grad_total[:, lanes]
        two_out[:, lanes] = state_v[1, :, lanes] + factor_two * grad_square[:, lanes]

    drain(squares_all.at[pl.ds(1, ndev - 1)], sq_send_sem)
    for j in range(nblock):
        lanes = slice(j * BLOCK, (j + 1) * BLOCK)
        projected = proj_own[:, lanes]
        drain(proj_recv.at[j], proj_recv_sem.at[j])
        for k in range(1, ngroup):
            projected = projected + proj_recv[j, k - 1].astype(jnp.float32)
        proj_out[:, lanes] = projected
    drain(proj_send, proj_send_sem)


def finish_kernel(
    one_ref,
    two_ref,
    proj_ref,
    cos_ref,
    sin_ref,
    query_ref,
    max_ref,
    sum_ref,
    old_ref,
    one_out,
    two_out,
    entries_out,
    attended_out,
    heads_v,
    entries_v,
    attended_v,
    one_sem,
    two_sem,
    entries_sem,
    attended_sem,
):
    rows = one_ref.shape[0]
    part = rows // 5
    for src, dst, sem in ((one_ref, one_out, one_sem), (two_ref, two_out, two_sem)):
        for i in range(5):
            here = pl.ds(i * part, part)
            pltpu.make_async_copy(src.at[here], dst.at[here], sem).start()
    nrow, nstep, cols = entries_out.shape
    tokens = nrow * nstep
    heads = cols // (2 * HD)
    groups = QH // KVH
    scaling = 1.0 / math.sqrt(HD)
    qi = lax.broadcasted_iota(jnp.int32, (nrow * PAD, tokens), 0)
    kj = lax.broadcasted_iota(jnp.int32, (nrow * PAD, tokens), 1)
    seen = (qi // PAD == kj // nstep) & (qi % nstep >= kj % nstep)
    new_keys, new_values = [], []
    for a in range(heads):
        k = proj_ref[:, 2 * a * HD : (2 * a + 1) * HD]
        k = k * cos_ref[...] + pltpu.roll(k, HD // 2, 1) * sin_ref[...]
        v = proj_ref[:, (2 * a + 1) * HD : (2 * a + 2) * HD]
        new_keys.append(k.astype(jnp.bfloat16))
        new_values.append(v.astype(jnp.bfloat16))
        for i in range(nrow):
            rows_i = slice(i * nstep, (i + 1) * nstep)
            entries_v[i, :, 2 * a * HD : (2 * a + 1) * HD] = k[rows_i].astype(jnp.bfloat16)
            entries_v[i, :, (2 * a + 1) * HD : (2 * a + 2) * HD] = v[rows_i].astype(jnp.bfloat16)
    pltpu.make_async_copy(entries_v, entries_out, entries_sem).start()
    for a in range(heads):
        scores = lax.dot_general(
            query_ref[a].astype(jnp.bfloat16), new_keys[a], (((1,), (1,)), ((), ())), preferred_element_type=jnp.float32
        )
        scores = jnp.where(seen, scores * scaling, NEG_FILL)
        before = max_ref[a][:, 0:1]
        top = jnp.maximum(before, jnp.max(scores, -1, keepdims=True))
        alpha = jnp.exp(before - top)
        e = jnp.exp(scores - top)
        whole = sum_ref[a][:, 0:1] * alpha + jnp.sum(e, -1, keepdims=True)
        o = old_ref[a] * alpha + jnp.dot(e.astype(jnp.bfloat16), new_values[a], preferred_element_type=jnp.float32)
        heads_v[a] = o / whole
        for i in range(nrow):
            for j in range(groups):
                n = a * groups + j
                at = i * PAD + j * nstep
                attended_v[i, :, n * HD : (n + 1) * HD] = heads_v[a, at : at + nstep, :].astype(jnp.bfloat16)
    pltpu.make_async_copy(attended_v, attended_out, attended_sem).start()
    for src, dst, sem in (
        (one_ref, one_out, one_sem),
        (two_ref, two_out, two_sem),
        (entries_v, entries_out, entries_sem),
        (attended_v, attended_out, attended_sem),
    ):
        pltpu.make_async_copy(src, dst, sem).wait()


def fused_body(
    sizes,
    grad_parts,
    master,
    moment_one,
    moment_two,
    hidden_in,
    queries,
    cache_keys,
    cache_values,
    cache_lengths,
):
    ngrp, nrep, ntp = sizes
    ngroup = ngrp * nrep
    ndev = ngroup * ntp
    rows, cols = master.shape
    nrow, nstep, width = hidden_in.shape
    tokens = nrow * nstep
    heads = cols // (2 * HD)
    plan = chunk_plan(rows)
    f32, bf16 = jnp.float32, jnp.bfloat16
    vm = pltpu.VMEM
    dma = pltpu.SemaphoreType.DMA
    vmem = pl.BlockSpec(memory_space=pltpu.VMEM)
    hbm = pl.BlockSpec(memory_space=pltpu.HBM)
    per_head = vm((heads, nrow * PAD, HD), f32)
    moment = vm((rows, cols), f32)
    table = vm((tokens, HD), f32)

    def with_local(*refs):
        def inner(*local):
            fused_kernel(sizes, *refs, *local)

        pl.run_scoped(inner, dma((nrow,)), *[pltpu.SemaphoreType.DMA] * 12)

    middle = pl.pallas_call(
        with_local,
        out_shape=(moment, moment, vm((tokens, cols), f32), table, table) + (per_head,) * 4,
        in_specs=[hbm] * 9,
        out_specs=(vmem,) * 9,
        scratch_shapes=[
            pltpu.SMEM((nrow,), jnp.int32),
            vm(queries.shape, bf16),
            vm((DIRECT, cols), f32),
            vm((DIRECT, cols), f32),
            vm((DIRECT, cols), bf16),
            vm((2, DIRECT, cols), bf16),
            vm((2 * rows, cols), f32),
            vm((rows, cols), bf16),
            vm((rows, cols), bf16),
            vm((2, rows, cols), f32),
            vm((rows, cols), f32),
            vm((rows, cols), f32),
            vm((rows, cols), f32),
            vm((3, rows, cols), f32),
            vm((nrow, 2) + cache_keys.shape[1:], bf16),
            vm((ngroup, nrow, nstep, rows), bf16),
            vm((ngroup * tokens, rows), f32),
            vm((ngroup * tokens, rows), bf16),
            vm((1, 128), f32),
            vm((ndev, 1, 128), f32),
            vm((tokens, cols), f32),
            vm((cols // BLOCK, ngroup - 1, tokens, BLOCK), bf16),
            vm((cols // BLOCK, ngroup - 1, tokens, BLOCK), bf16),
            dma((len(plan),)),
            dma((len(plan),)),
            dma((cols // BLOCK,)),
        ]
        + [pltpu.SemaphoreType.DMA] * 4
        + [pltpu.SemaphoreType.REGULAR((ndev.bit_length() - 1,))],
        compiler_params=pltpu.CompilerParams(
            collective_id=0, has_side_effects=True, vmem_limit_bytes=60 * 1024 * 1024 + 320 * 1024
        ),
    )(cache_lengths, hidden_in, queries, grad_parts, master, moment_one, moment_two, cache_keys, cache_values)
    return pl.pallas_call(
        finish_kernel,
        out_shape=(
            jax.ShapeDtypeStruct((rows, cols), f32),
            jax.ShapeDtypeStruct((rows, cols), f32),
            jax.ShapeDtypeStruct((nrow, nstep, cols), bf16),
            jax.ShapeDtypeStruct(queries.shape, bf16),
        ),
        in_specs=[vmem] * 9,
        out_specs=(hbm,) * 4,
        scratch_shapes=[vm((heads, nrow * PAD, HD), f32), vm((nrow, nstep, cols), bf16), vm(queries.shape, bf16)]
        + [pltpu.SemaphoreType.DMA] * 4,
        compiler_params=pltpu.CompilerParams(vmem_limit_bytes=8 * 1024 * 1024),
    )(*middle)


def solution(mesh):
    sizes = (mesh.shape["grp"], mesh.shape["rep"], mesh.shape["tp"])
    fits = sizes[2] == 4 and D % (sizes[0] * sizes[1] * 128) == 0 and KVH % sizes[2] == 0
    fits = fits and (sizes[0] * sizes[1]) & (sizes[0] * sizes[1] - 1) == 0
    placed = (
        P("tp", ("grp", "rep"), None),
        P(("grp", "rep"), "tp"),
        P(("grp", "rep"), "tp"),
        P(("grp", "rep"), "tp"),
        P(("grp", "rep"), None, None),
        P(("grp", "rep"), None, "tp"),
        P(("grp", "rep"), None, "tp"),
        P(("grp", "rep"), None, "tp"),
        P(("grp", "rep")),
    )
    return jax.shard_map(
        functools.partial(fused_body, sizes) if fits else body,
        mesh=mesh,
        in_specs=placed,
        out_specs=(
            P(("grp", "rep"), "tp"),
            P(("grp", "rep"), "tp"),
            P(("grp", "rep"), None, "tp"),
            P(("grp", "rep"), None, "tp"),
        ),
        check_vma=False,
    )
```

```python
import functools
import math

import jax
import jax.numpy as jnp
from jax import lax
from jax.experimental import pallas as pl
from jax.experimental.pallas import tpu as pltpu
from jax.sharding import PartitionSpec as P

D = 5120
QH = 40
KVH = 8
HD = 128


BETA_ONE = 0.9
BETA_TWO = 0.999
FIRST_CORR = 0.9999734386011124
SECOND_CORR = 0.09520785288629041
LEARN_RATE = 0.003
EPSILON = 1e-08
ROPE_BASE = 1000000.0
NEG_FILL = -1e30


def rotate(new_keys, lengths):
    positions = (lengths[:, None] + jnp.arange(new_keys.shape[1], dtype=jnp.int32)[None, :]).astype(
        jnp.float32
    )
    half_dim = new_keys.shape[-1] // 2
    inverse = jnp.exp(
        -math.log(ROPE_BASE) * 2.0 * jnp.arange(half_dim, dtype=jnp.float32) / new_keys.shape[-1]
    )
    angles = positions[:, :, None] * inverse[None, None, :]
    cosine_part = jnp.concatenate([jnp.cos(angles), jnp.cos(angles)], -1)[:, :, None, :]
    sine_part = jnp.concatenate([jnp.sin(angles), jnp.sin(angles)], -1)[:, :, None, :]
    rotated = jnp.concatenate([-new_keys[..., half_dim:], new_keys[..., :half_dim]], -1)
    return new_keys * cosine_part + rotated * sine_part


def body(
    grad_parts,
    master,
    moment_one,
    moment_two,
    hidden_in,
    queries,
    cache_keys,
    cache_values,
    cache_lengths,
):
    col_width = master.shape[1]
    grad_sum = lax.psum_scatter(grad_parts[0], "tp", scatter_dimension=1, tiled=True)
    squares = lax.psum(jnp.sum(grad_sum * grad_sum), ("grp", "rep", "tp"))
    norm_limit = math.sqrt(D * 2 * KVH * HD)
    clipped = grad_sum * jnp.minimum(1.0, norm_limit / jnp.sqrt(squares))
    new_moment_one = BETA_ONE * moment_one + (1.0 - BETA_ONE) * clipped
    new_moment_two = BETA_TWO * moment_two + (1.0 - BETA_TWO) * clipped * clipped
    update = new_moment_one / FIRST_CORR / (jnp.sqrt(new_moment_two / SECOND_CORR) + EPSILON)
    weights = (master - LEARN_RATE * update).astype(jnp.bfloat16)
    row_count, step_count, model_width = hidden_in.shape
    token_count = row_count * step_count
    flat_inputs = hidden_in.reshape(token_count, model_width)
    sliced = lax.all_to_all(
        lax.all_to_all(flat_inputs, "grp", split_axis=1, concat_axis=0, tiled=True),
        "rep",
        split_axis=1,
        concat_axis=0,
        tiled=True,
    )
    group_count = lax.axis_size("grp")
    replica_count = lax.axis_size("rep")
    ordered = sliced.reshape(replica_count, group_count, token_count, weights.shape[0])
    ordered = jnp.swapaxes(ordered, 0, 1).reshape(
        group_count * replica_count * token_count, weights.shape[0]
    )
    projected = lax.psum_scatter(
        jnp.dot(ordered, weights, preferred_element_type=jnp.float32),
        ("grp", "rep"),
        scatter_dimension=0,
        tiled=True,
    )
    heads_here = col_width // (2 * HD)
    projected = projected.reshape(row_count, step_count, heads_here, 2, HD)
    new_keys = rotate(projected[:, :, :, 0, :], cache_lengths).astype(jnp.bfloat16)
    new_values = projected[:, :, :, 1, :].astype(jnp.bfloat16)
    new_entries = jnp.stack([new_keys, new_values], 3).reshape(row_count, step_count, col_width)
    groups = QH // KVH
    slots = cache_keys.shape[1]
    query_heads = queries.reshape(row_count, step_count, heads_here, groups, HD)
    old_k = cache_keys.reshape(row_count, slots, heads_here, HD)
    old_v = cache_values.reshape(row_count, slots, heads_here, HD)
    scaling = 1.0 / math.sqrt(HD)
    old_scores = (
        jnp.einsum("rsagd,rjad->rsagj", query_heads, old_k, preferred_element_type=jnp.float32)
        * scaling
    )
    valid_slots = jnp.arange(slots, dtype=jnp.int32)[None, :] < cache_lengths[:, None]
    old_scores = jnp.where(valid_slots[:, None, None, None, :], old_scores, NEG_FILL)
    new_scores = (
        jnp.einsum("rsagd,rtad->rsagt", query_heads, new_keys, preferred_element_type=jnp.float32)
        * scaling
    )
    causal = jnp.arange(step_count)[:, None] >= jnp.arange(step_count)[None, :]
    new_scores = jnp.where(causal[None, :, None, None, :], new_scores, NEG_FILL)
    scores = jnp.concatenate([old_scores, new_scores], -1)
    row_max = jnp.max(scores, -1, keepdims=True)
    exp_scores = jnp.exp(scores - row_max)
    probs = (exp_scores / jnp.sum(exp_scores, -1, keepdims=True)).astype(jnp.bfloat16)
    output = jnp.einsum(
        "rsagj,rjad->rsagd", probs[..., :slots], old_v, preferred_element_type=jnp.float32
    )
    output = output + jnp.einsum(
        "rsagt,rtad->rsagd", probs[..., slots:], new_values, preferred_element_type=jnp.float32
    )
    attended = output.reshape(row_count, step_count, heads_here * groups * HD).astype(jnp.bfloat16)
    return (new_moment_one, new_moment_two, new_entries, attended)


MESH = pl.DeviceIdType.MESH
PAD = 32
BLOCK = 256
DIRECT = 64
STEP_SIZE = LEARN_RATE / FIRST_CORR * math.sqrt(SECOND_CORR)
STEP_EPSILON = EPSILON * math.sqrt(SECOND_CORR)


def chunk_plan(rows):
    sizes = [DIRECT // 2, DIRECT // 2, DIRECT // 2, DIRECT // 2, 64]
    left = rows - sum(sizes) - 32
    while left > 0:
        sizes.append(min(192, left))
        left -= sizes[-1]
    sizes.append(32)
    return [(sum(sizes[:i]), n) for i, n in enumerate(sizes)]


def fused_kernel(
    sizes,
    lengths_ref,
    hidden_ref,
    queries_ref,
    grad_ref,
    master_ref,
    one_ref,
    two_ref,
    keys_ref,
    values_ref,
    one_out,
    two_out,
    proj_out,
    cos_out,
    sin_out,
    query_f,
    old_max,
    old_sum,
    old_out,
    lengths_s,
    queries_v,
    mate_src,
    direct_src,
    direct_send,
    direct_in,
    fwd_in,
    fwd_send,
    sum_far,
    sum_in,
    grad_total,
    grad_square,
    step_v,
    share_v,
    share_square,
    state_v,
    cache_v,
    hidden_in_v,
    hidden_f,
    hidden_b,
    squares_send,
    squares_all,
    proj_own,
    proj_send,
    proj_recv,
    proj_count,
    fwd_sem,
    far_recv_sem,
    proj_recv_sem,
    sum_sem,
    direct_recv_sem,
    hid_recv_sem,
    sq_recv_sem,
    share_recv_sem,
    round_sem,
    cache_sem,
    early_sem,
    first_sem,
    direct_send_sem,
    mate_send_sem,
    far_send_sem,
    hid_send_sem,
    sq_send_sem,
    proj_send_sem,
    load_sem,
    length_sem,
    query_sem,
    own_sem,
    share_send_sem,
):
    ngrp, nrep, ntp = sizes
    ngroup = ngrp * nrep
    ndev = ngroup * ntp
    rows, cols = master_ref.shape
    nrow, nstep, width = hidden_ref.shape
    tokens = nrow * nstep
    slots = keys_ref.shape[1]
    heads = cols // (2 * HD)
    groups = QH // KVH
    plan = chunk_plan(rows)
    nchunk = len(plan)
    nblock = cols // BLOCK
    scaling = 1.0 / math.sqrt(HD)

    g = lax.axis_index("grp")
    r = lax.axis_index("rep")
    t = lax.axis_index("tp")
    p = g * nrep + r
    y = t // 2
    c = t % 2
    mate = y * 2 + (1 - c)
    far = (1 - y) * 2 + c
    far_mate = (1 - y) * 2 + (1 - c)

    def toggles(v, size):
        return [(1 << b) * (1 - 2 * lax.rem(lax.div(v, 1 << b), 2)) for b in range(size.bit_length() - 1)]

    flips = {"grp": toggles(g, ngrp), "rep": toggles(r, nrep), "tp": toggles(t, ntp)}
    base = {"grp": g, "rep": r, "tp": t}

    def peer(**bits):
        return {
            name: base[name] + sum(d for b, d in enumerate(flips[name]) if bits.get(name, 0) >> b & 1)
            for name in base
        }

    def group_bits(k):
        return {"grp": k // nrep, "rep": k % nrep}

    def group_peer(k):
        return peer(**group_bits(k))

    def flat_bits(k):
        return {"tp": k % ntp, **group_bits(k // ntp)}

    def hops(k):
        bits = flat_bits(k)
        return bits["grp"] + bits["rep"] + bits["tp"] // 2 + 0.3 * (bits["tp"] % 2)

    flat_order = sorted(range(1, ndev), key=hops, reverse=True)
    group_order = sorted(range(1, ngroup), key=lambda k: hops(k * ntp), reverse=True)

    barrier = pltpu.get_barrier_semaphore()
    bits = ndev.bit_length() - 1

    def across(b):
        return peer(**flat_bits(1 << b))

    for b in range(bits):
        pl.semaphore_signal(barrier, inc=1, device_id=across(b), device_id_type=MESH)
    pl.semaphore_signal(barrier, inc=1, device_id=peer(tp=3), device_id_type=MESH)

    def block(start, n, owner):
        return grad_ref.at[0, pl.ds(start, n), pl.ds(pl.multiple_of(owner * cols, cols), cols)]

    def drain(ref, sem):
        pltpu.make_async_copy(ref, ref, sem).wait()

    target = (1 - y) * 2
    direct_copy = pltpu.make_async_copy(block(0, DIRECT, target), direct_src, first_sem)
    early_start = pl.multiple_of(c * DIRECT, DIRECT)
    early_copy = pltpu.make_async_copy(block(early_start, DIRECT, far_mate), mate_src, early_sem)
    early_copy.start()
    direct_copy.start()

    direct_put = pltpu.make_async_remote_copy(
        src_ref=direct_send,
        dst_ref=direct_in.at[c],
        send_sem=direct_send_sem,
        recv_sem=direct_recv_sem,
        device_id={**base, "tp": target},
        device_id_type=MESH,
    )

    def early_mate(i):
        half = DIRECT // 2
        return pltpu.make_async_remote_copy(
            src_ref=mate_src.at[pl.ds(i * half, half)],
            dst_ref=fwd_in.at[pl.ds(pl.multiple_of(2 * (early_start + i * half) + half, half), half)],
            send_sem=mate_send_sem,
            recv_sem=fwd_sem.at[2 * c + i],
            device_id=peer(tp=1),
            device_id_type=MESH,
        )

    def own_copy(i):
        start, n = plan[i]
        return pltpu.make_async_copy(block(start, n, far), fwd_in.at[pl.ds(2 * start, n)], fwd_sem.at[i])

    def mate_copy(i):
        start, n = plan[i]
        return pltpu.make_async_remote_copy(
            src_ref=block(start, n, far_mate),
            dst_ref=fwd_in.at[pl.ds(2 * start + n, n)],
            send_sem=mate_send_sem,
            recv_sem=fwd_sem.at[i],
            device_id=peer(tp=1),
            device_id_type=MESH,
        )

    def far_copy(i):
        start, n = plan[i]
        return pltpu.make_async_remote_copy(
            src_ref=fwd_send.at[pl.ds(start, n)],
            dst_ref=sum_far.at[pl.ds(start, n)],
            send_sem=far_send_sem,
            recv_sem=far_recv_sem.at[i],
            device_id=peer(tp=2),
            device_id_type=MESH,
        )

    def hid_copy(k):
        to = group_peer(k)
        q = to["grp"] * nrep + to["rep"]
        return pltpu.make_async_remote_copy(
            src_ref=hidden_ref.at[:, :, pl.ds(pl.multiple_of(q * rows, 128), rows)],
            dst_ref=hidden_in_v.at[k],
            send_sem=hid_send_sem,
            recv_sem=hid_recv_sem,
            device_id=to,
            device_id_type=MESH,
        )

    def sq_copy(k):
        return pltpu.make_async_remote_copy(
            src_ref=squares_send,
            dst_ref=squares_all.at[k],
            send_sem=sq_send_sem,
            recv_sem=sq_recv_sem,
            device_id=peer(**flat_bits(k)),
            device_id_type=MESH,
        )

    def proj_copy(j, k, shared=False):
        return pltpu.make_async_remote_copy(
            src_ref=proj_send.at[nblock if shared else j, k],
            dst_ref=proj_recv.at[j, k],
            send_sem=proj_send_sem,
            recv_sem=proj_recv_sem.at[j],
            device_id=peer(tp=1, **group_bits(k)) if shared else group_peer(k),
            device_id_type=MESH,
        )

    def share_copy(i):
        src = (one_ref, two_ref, master_ref, grad_total)[i]
        return pltpu.make_async_remote_copy(
            src_ref=src.at[:, pl.ds(0, BLOCK)],
            dst_ref=share_v.at[i],
            send_sem=share_send_sem,
            recv_sem=share_recv_sem,
            device_id=peer(tp=1),
            device_id_type=MESH,
        )

    length_copy = pltpu.make_async_copy(lengths_ref, lengths_s, length_sem)
    query_copy = pltpu.make_async_copy(queries_ref, queries_v, query_sem)
    own_hidden = pltpu.make_async_copy(
        hidden_ref.at[:, :, pl.ds(pl.multiple_of(p * rows, 128), rows)], hidden_in_v.at[0], own_sem
    )

    early_copy.wait()
    pl.semaphore_wait(barrier, bits + 1)

    early_mate(0).start()
    early_mate(1).start()
    direct_copy.wait()
    direct_send[...] = direct_src[...].astype(jnp.bfloat16)
    direct_put.start()

    @pl.when(c == 1)
    def _():
        own_copy(0).start()
        own_copy(1).start()

    for i in range(2, nchunk):
        own_copy(i).start()

    @pl.when(c == 0)
    def _():
        mate_copy(2).start()
        mate_copy(3).start()

    for i in range(4, nchunk):
        mate_copy(i).start()
    pltpu.make_async_remote_copy(
        src_ref=block(0, rows, mate),
        dst_ref=sum_in.at[1],
        send_sem=mate_send_sem,
        recv_sem=sum_sem,
        device_id=peer(tp=1),
        device_id_type=MESH,
    ).start()

    @pl.when(c == 0)
    def _():
        for i in range(3):
            share_copy(i).start()

    for copy in (length_copy, query_copy, own_hidden):
        copy.start()
    for i in range(nrow):
        pltpu.make_async_copy(keys_ref.at[i], cache_v.at[i, 0], cache_sem.at[i]).start()
        pltpu.make_async_copy(values_ref.at[i], cache_v.at[i, 1], cache_sem.at[i]).start()
    pltpu.make_async_copy(block(0, rows, t), sum_in.at[0], sum_sem).start()
    for i, src in enumerate((one_ref, two_ref, master_ref)):
        pltpu.make_async_copy(src, state_v.at[i], load_sem).start()

    def forward(i):
        start, n = plan[i]
        drain(fwd_in.at[pl.ds(2 * start, 2 * n)], fwd_sem.at[i])
        fwd_send[start : start + n, :] = (
            fwd_in[2 * start : 2 * start + n, :] + fwd_in[2 * start + n : 2 * start + 2 * n, :]
        ).astype(jnp.bfloat16)
        far_copy(i).start()

    for b in range(bits):
        pl.semaphore_signal(round_sem.at[b], inc=1, device_id=across(b), device_id_type=MESH)
        for i in range(b * nchunk // bits, (b + 1) * nchunk // bits):
            if i < 2:
                pl.when(c == 1)(functools.partial(forward, i))
            else:
                forward(i)
        pl.semaphore_wait(round_sem.at[b], 1)
    for k in group_order:
        hid_copy(k).start()

    for copy in (length_copy, query_copy):
        copy.wait()
    query_f[...] = jnp.zeros_like(query_f)
    for i in range(nrow):
        row_q = queries_v[i].astype(jnp.float32)
        for a in range(heads):
            for j in range(groups):
                n = a * groups + j
                query_f[a, i * PAD + j * nstep : i * PAD + (j + 1) * nstep, :] = row_q[:, n * HD : (n + 1) * HD]

    slot = lax.broadcasted_iota(jnp.int32, (PAD, slots), 1)
    for i in range(nrow):
        drain(cache_v.at[i], cache_sem.at[i])
        valid = slot < lengths_s[i]
        for a in range(heads):
            q = query_f[a, i * PAD : (i + 1) * PAD, :].astype(jnp.bfloat16)
            scores = lax.dot_general(
                q,
                cache_v[i, 0, :, a * HD : (a + 1) * HD],
                (((1,), (1,)), ((), ())),
                preferred_element_type=jnp.float32,
            )
            scores = jnp.where(valid, scores * scaling, NEG_FILL)
            top = jnp.max(scores, -1, keepdims=True)
            e = jnp.exp(scores - top)
            here = slice(i * PAD, (i + 1) * PAD)
            old_max[a, here, :] = jnp.broadcast_to(top, (PAD, HD))
            old_sum[a, here, :] = jnp.broadcast_to(jnp.sum(e, -1, keepdims=True), (PAD, HD))
            old_out[a, here, :] = jnp.dot(
                e.astype(jnp.bfloat16), cache_v[i, 1, :, a * HD : (a + 1) * HD], preferred_element_type=jnp.float32
            )

    token = lax.broadcasted_iota(jnp.int32, (tokens, HD), 0)
    lane = lax.broadcasted_iota(jnp.int32, (tokens, HD), 1)
    position = lax.rem(token, nstep)
    for i in range(nrow):
        position = position + jnp.where(token // nstep == i, lengths_s[i], 0)
    pair = lax.rem(lane, HD // 2).astype(jnp.float32)
    angle = position.astype(jnp.float32) * jnp.exp(-math.log(ROPE_BASE) * 2.0 * pair / HD)
    cos_out[...] = jnp.cos(angle)
    sin_out[...] = jnp.where(lane < HD // 2, -jnp.sin(angle), jnp.sin(angle))

    drain(state_v, load_sem)

    def prescale(i, carry):
        here = pl.ds(pl.multiple_of(i * 64, 64), 64)
        step_v[here, :] = (BETA_ONE * STEP_SIZE) * state_v[0, here, :]
        state_v[1, here, :] = BETA_TWO * state_v[1, here, :]
        return carry

    lax.fori_loop(0, rows // 64, prescale, 0)

    own_hidden.wait()
    drain(hidden_in_v.at[pl.ds(1, ngroup - 1)], hid_recv_sem)
    for k in range(ngroup):
        own = hidden_in_v[k]
        for i in range(nrow):
            at = k * tokens + i * nstep
            hidden_f[at : at + nstep, :] = own[i].astype(jnp.float32)
    hidden_b[...] = hidden_f[...].astype(jnp.bfloat16)

    drain(sum_in, sum_sem)

    @pl.when(c == 0)
    def _():
        drain(direct_in, direct_recv_sem)
        sum_in[0, :DIRECT, :] = (
            sum_in[0, :DIRECT, :] + direct_in[0].astype(jnp.float32) + direct_in[1].astype(jnp.float32)
        )
        sum_far[:DIRECT, :] = jnp.zeros((DIRECT, cols), jnp.bfloat16)

    @pl.when(c == 1)
    def _():
        for i in range(2):
            start, n = plan[i]
            drain(sum_far.at[pl.ds(start, n)], far_recv_sem.at[i])

    acc = jnp.zeros((8, cols), jnp.float32)
    for i, (start, n) in enumerate(plan):
        here = slice(start, start + n)
        if i > 1:
            drain(sum_far.at[pl.ds(start, n)], far_recv_sem.at[i])
        s = sum_in[0, here, :] + sum_in[1, here, :] + sum_far[here, :].astype(jnp.float32)
        grad_total[here, :] = s
        square = s * s
        grad_square[here, :] = square
        acc = acc + jnp.sum(square.reshape(n // 8, 8, cols), axis=0)
    mine = jnp.sum(sum(acc[:, j * 128 : (j + 1) * 128] for j in range(cols // 128)), axis=0, keepdims=True)
    squares_send[...] = mine
    for k in flat_order:
        sq_copy(k).start()
    squares_all[0] = mine

    @pl.when(c == 0)
    def _():
        share_copy(3).start()

    @pl.when(c == 1)
    def _():
        drain(share_v, share_recv_sem)

        def prepare(i, carry):
            here = pl.ds(pl.multiple_of(i * 64, 64), 64)
            share_v[0, here, :] = (BETA_ONE * STEP_SIZE) * share_v[0, here, :]
            share_v[1, here, :] = BETA_TWO * share_v[1, here, :]
            share_square[here, :] = share_v[3, here, :] * share_v[3, here, :]
            return carry

        lax.fori_loop(0, rows // 64, prepare, 0)

    drain(direct_send, direct_send_sem)

    @pl.when(c == 0)
    def _():
        drain(fwd_in, mate_send_sem)
        drain(fwd_send.at[pl.ds(DIRECT, rows - DIRECT)], far_send_sem)

    @pl.when(c == 1)
    def _():
        drain(fwd_in.at[pl.ds(DIRECT, 2 * rows - DIRECT)], mate_send_sem)
        drain(fwd_send, far_send_sem)

    drain(hidden_in_v.at[pl.ds(1, ngroup - 1)], hid_send_sem)
    drain(squares_all.at[pl.ds(1, ndev - 1)], sq_recv_sem)
    squares = jnp.sum(jnp.sum(squares_all[...], axis=0), axis=1, keepdims=True)
    norm_limit = math.sqrt(D * 2 * KVH * HD)
    factor = jnp.minimum(1.0, norm_limit / jnp.sqrt(jnp.broadcast_to(squares, (1, BLOCK))))
    factor_step = ((1.0 - BETA_ONE) * STEP_SIZE) * factor
    factor_two = (1.0 - BETA_TWO) * factor * factor

    def weights(step, two, grad, square, old):
        step = step + factor_step * grad
        two = two + factor_two * square
        return (old - step / (two * lax.rsqrt(two) + STEP_EPSILON)).astype(jnp.bfloat16)

    def project(w):
        return jnp.dot(hidden_b[...], w, preferred_element_type=jnp.float32)

    def shared_block():
        partial = project(weights(share_v[0], share_v[1], share_v[3], share_square[...], share_v[2]))
        for k in group_order + [0]:
            proj_send[nblock, k] = partial[k * tokens : (k + 1) * tokens].astype(jnp.bfloat16)
        for k in group_order + [0]:
            proj_copy(0, k, True).start()

    def block_of(j):
        lanes = slice(j * BLOCK, (j + 1) * BLOCK)
        partial = project(
            weights(
                step_v[:, lanes], state_v[1, :, lanes], grad_total[:, lanes], grad_square[:, lanes], state_v[2, :, lanes]
            )
        )
        for k in group_order:
            proj_send[j, k] = partial[k * tokens : (k + 1) * tokens].astype(jnp.bfloat16)
        for k in group_order:
            proj_copy(j, k).start()
        proj_own[:, lanes] = partial[0:tokens]

    @pl.when(c == 1)
    def _():
        for j in range(nblock):
            block_of(j)
        shared_block()

    @pl.when(c == 0)
    def _():
        for j in range(1, nblock):
            block_of(j)

    factor_one = (1.0 - BETA_ONE) * factor
    for j in range(nblock):
        lanes = slice(j * BLOCK, (j + 1) * BLOCK)
        one_out[:, lanes] = BETA_ONE * state_v[0, :, lanes] + factor_one * grad_total[:, lanes]
        two_out[:, lanes] = state_v[1, :, lanes] + factor_two * grad_square[:, lanes]

    drain(squares_all.at[pl.ds(1, ndev - 1)], sq_send_sem)
    for j in range(nblock):
        lanes = slice(j * BLOCK, (j + 1) * BLOCK)
        if j == 0:
            @pl.when(c == 0)
            def _():
                drain(proj_recv.at[0], proj_recv_sem.at[0])
                proj_own[:, lanes] = proj_recv[0, 0].astype(jnp.float32)

            @pl.when(c == 1)
            def _():
                drain(proj_recv.at[0, pl.ds(1, ngroup - 1)], proj_recv_sem.at[0])

        else:
            drain(proj_recv.at[j, pl.ds(1, ngroup - 1)], proj_recv_sem.at[j])
        projected = proj_own[:, lanes]
        for k in range(1, ngroup):
            projected = projected + proj_recv[j, k].astype(jnp.float32)
        proj_out[:, lanes] = projected

    @pl.when(c == 0)
    def _():
        drain(share_v, share_send_sem)
        drain(proj_recv.at[pl.ds(1, nblock - 1), pl.ds(1, ngroup - 1)], proj_send_sem)

    @pl.when(c == 1)
    def _():
        drain(proj_count.at[pl.ds(0, nblock * (ngroup - 1) + ngroup)], proj_send_sem)


def finish_kernel(
    one_ref,
    two_ref,
    proj_ref,
    cos_ref,
    sin_ref,
    query_ref,
    max_ref,
    sum_ref,
    old_ref,
    one_out,
    two_out,
    entries_out,
    attended_out,
    heads_v,
    entries_v,
    attended_v,
    one_sem,
    two_sem,
    entries_sem,
    attended_sem,
):
    rows = one_ref.shape[0]
    part = rows // 5
    for src, dst, sem in ((one_ref, one_out, one_sem), (two_ref, two_out, two_sem)):
        for i in range(5):
            here = pl.ds(i * part, part)
            pltpu.make_async_copy(src.at[here], dst.at[here], sem).start()
    nrow, nstep, cols = entries_out.shape
    tokens = nrow * nstep
    heads = cols // (2 * HD)
    groups = QH // KVH
    scaling = 1.0 / math.sqrt(HD)
    qi = lax.broadcasted_iota(jnp.int32, (nrow * PAD, tokens), 0)
    kj = lax.broadcasted_iota(jnp.int32, (nrow * PAD, tokens), 1)
    seen = (qi // PAD == kj // nstep) & (qi % nstep >= kj % nstep)
    new_keys, new_values = [], []
    for a in range(heads):
        k = proj_ref[:, 2 * a * HD : (2 * a + 1) * HD]
        k = k * cos_ref[...] + pltpu.roll(k, HD // 2, 1) * sin_ref[...]
        v = proj_ref[:, (2 * a + 1) * HD : (2 * a + 2) * HD]
        new_keys.append(k.astype(jnp.bfloat16))
        new_values.append(v.astype(jnp.bfloat16))
        for i in range(nrow):
            rows_i = slice(i * nstep, (i + 1) * nstep)
            entries_v[i, :, 2 * a * HD : (2 * a + 1) * HD] = k[rows_i].astype(jnp.bfloat16)
            entries_v[i, :, (2 * a + 1) * HD : (2 * a + 2) * HD] = v[rows_i].astype(jnp.bfloat16)
    pltpu.make_async_copy(entries_v, entries_out, entries_sem).start()
    for a in range(heads):
        scores = lax.dot_general(
            query_ref[a].astype(jnp.bfloat16), new_keys[a], (((1,), (1,)), ((), ())), preferred_element_type=jnp.float32
        )
        scores = jnp.where(seen, scores * scaling, NEG_FILL)
        before = max_ref[a][:, 0:1]
        top = jnp.maximum(before, jnp.max(scores, -1, keepdims=True))
        alpha = jnp.exp(before - top)
        e = jnp.exp(scores - top)
        whole = sum_ref[a][:, 0:1] * alpha + jnp.sum(e, -1, keepdims=True)
        o = old_ref[a] * alpha + jnp.dot(e.astype(jnp.bfloat16), new_values[a], preferred_element_type=jnp.float32)
        heads_v[a] = o / whole
        for i in range(nrow):
            for j in range(groups):
                n = a * groups + j
                at = i * PAD + j * nstep
                attended_v[i, :, n * HD : (n + 1) * HD] = heads_v[a, at : at + nstep, :].astype(jnp.bfloat16)
    pltpu.make_async_copy(attended_v, attended_out, attended_sem).start()
    for src, dst, sem in (
        (one_ref, one_out, one_sem),
        (two_ref, two_out, two_sem),
        (entries_v, entries_out, entries_sem),
        (attended_v, attended_out, attended_sem),
    ):
        pltpu.make_async_copy(src, dst, sem).wait()


def fused_body(
    sizes,
    grad_parts,
    master,
    moment_one,
    moment_two,
    hidden_in,
    queries,
    cache_keys,
    cache_values,
    cache_lengths,
):
    ngrp, nrep, ntp = sizes
    ngroup = ngrp * nrep
    ndev = ngroup * ntp
    rows, cols = master.shape
    nrow, nstep, width = hidden_in.shape
    tokens = nrow * nstep
    heads = cols // (2 * HD)
    plan = chunk_plan(rows)
    f32, bf16 = jnp.float32, jnp.bfloat16
    vm = pltpu.VMEM
    dma = pltpu.SemaphoreType.DMA
    vmem = pl.BlockSpec(memory_space=pltpu.VMEM)
    hbm = pl.BlockSpec(memory_space=pltpu.HBM)
    per_head = vm((heads, nrow * PAD, HD), f32)
    moment = vm((rows, cols), f32)
    table = vm((tokens, HD), f32)

    def with_local(*refs):
        def inner(*local):
            fused_kernel(sizes, *refs, *local)

        pl.run_scoped(inner, dma((nrow,)), *[pltpu.SemaphoreType.DMA] * 13)

    middle = pl.pallas_call(
        with_local,
        out_shape=(moment, moment, vm((tokens, cols), f32), table, table) + (per_head,) * 4,
        in_specs=[hbm] * 9,
        out_specs=(vmem,) * 9,
        scratch_shapes=[
            pltpu.SMEM((nrow,), jnp.int32),
            vm(queries.shape, bf16),
            vm((DIRECT, cols), f32),
            vm((DIRECT, cols), f32),
            vm((DIRECT, cols), bf16),
            vm((2, DIRECT, cols), bf16),
            vm((2 * rows, cols), f32),
            vm((rows, cols), bf16),
            vm((rows, cols), bf16),
            vm((2, rows, cols), f32),
            vm((rows, cols), f32),
            vm((rows, cols), f32),
            vm((rows, cols), f32),
            vm((4, rows, BLOCK), f32),
            vm((rows, BLOCK), f32),
            vm((3, rows, cols), f32),
            vm((nrow, 2) + cache_keys.shape[1:], bf16),
            vm((ngroup, nrow, nstep, rows), bf16),
            vm((ngroup * tokens, rows), f32),
            vm((ngroup * tokens, rows), bf16),
            vm((1, 128), f32),
            vm((ndev, 1, 128), f32),
            vm((tokens, cols), f32),
            vm((cols // BLOCK + 1, ngroup, tokens, BLOCK), bf16),
            vm((cols // BLOCK, ngroup, tokens, BLOCK), bf16),
            vm((cols // BLOCK * (ngroup - 1) + ngroup, tokens, BLOCK), bf16),
            dma((len(plan),)),
            dma((len(plan),)),
            dma((cols // BLOCK,)),
        ]
        + [pltpu.SemaphoreType.DMA] * 5
        + [pltpu.SemaphoreType.REGULAR((ndev.bit_length() - 1,))],
        compiler_params=pltpu.CompilerParams(
            collective_id=0, has_side_effects=True, vmem_limit_bytes=60 * 1024 * 1024 + 320 * 1024
        ),
    )(cache_lengths, hidden_in, queries, grad_parts, master, moment_one, moment_two, cache_keys, cache_values)
    return pl.pallas_call(
        finish_kernel,
        out_shape=(
            jax.ShapeDtypeStruct((rows, cols), f32),
            jax.ShapeDtypeStruct((rows, cols), f32),
            jax.ShapeDtypeStruct((nrow, nstep, cols), bf16),
            jax.ShapeDtypeStruct(queries.shape, bf16),
        ),
        in_specs=[vmem] * 9,
        out_specs=(hbm,) * 4,
        scratch_shapes=[vm((heads, nrow * PAD, HD), f32), vm((nrow, nstep, cols), bf16), vm(queries.shape, bf16)]
        + [pltpu.SemaphoreType.DMA] * 4,
        compiler_params=pltpu.CompilerParams(vmem_limit_bytes=8 * 1024 * 1024),
    )(*middle)


def solution(mesh):
    sizes = (mesh.shape["grp"], mesh.shape["rep"], mesh.shape["tp"])
    fits = sizes[2] == 4 and D % (sizes[0] * sizes[1] * 128) == 0 and KVH % sizes[2] == 0
    fits = fits and (sizes[0] * sizes[1]) & (sizes[0] * sizes[1] - 1) == 0
    placed = (
        P("tp", ("grp", "rep"), None),
        P(("grp", "rep"), "tp"),
        P(("grp", "rep"), "tp"),
        P(("grp", "rep"), "tp"),
        P(("grp", "rep"), None, None),
        P(("grp", "rep"), None, "tp"),
        P(("grp", "rep"), None, "tp"),
        P(("grp", "rep"), None, "tp"),
        P(("grp", "rep")),
    )
    return jax.shard_map(
        functools.partial(fused_body, sizes) if fits else body,
        mesh=mesh,
        in_specs=placed,
        out_specs=(
            P(("grp", "rep"), "tp"),
            P(("grp", "rep"), "tp"),
            P(("grp", "rep"), None, "tp"),
            P(("grp", "rep"), None, "tp"),
        ),
        check_vma=False,
    )
```
